128 devices in a mesh: row: 16 (over y, x), col: 8 (over z, core).
Axes of the slice: x: 4, y: 4, z: 4, core: 2. Of those that a mesh axis runs over, the one named last changes fastest.
Arguments:
- moments: float32 [2, 128, 128, 6144], P(None, None, 'row', 'col'), may hold values from -6 to 6
- owner_counts: int32 [16], replicated, may hold values from 1 to 16, 128 in all
Outputs:
- normalized: float32 [2, 32768, 6144], P(None, 'row', 'col')
- scales: float32 [2, 256], P(None, 'row')
- energy: float32 [2, 256], P(None, 'row')
The draws below stay inside these ranges and needn't reach their ends.
Inputs may be any that keep to these rules, and one draw needn't show every extreme that they name: owner_counts sums to 128, and its largest entry is exactly 16.
All inputs are finite; a program needn't handle non-finite values.
Results may differ from the reference program's by a relative error of at most 0.00002.
Values sent between devices are 32-bit elements.
A program may use at most 128 MiB of HBM per device.

```python
import math
import jax
import jax.numpy as jnp
import numpy as np
from jax import lax

D = 6144
BLK = 128
TENSORS = 2
NB = 128
MOST = 16
N_ROW = 16


def level_of(rng, extent, cuts, smallest, largest):
    factor_of = 1.0
    for position, blocks in cuts:
        steps = jax.random.uniform(jax.random.fold_in(jax.random.fold_in(rng, 6), position), (blocks,), jnp.float32, smallest / len(cuts), largest / len(cuts))
        factor_of = factor_of * jnp.repeat(jnp.exp(steps), extent[position] // blocks).reshape((-1,) + (1,) * (len(extent) - 1 - position))
    return factor_of


def profile(amount, total, bound, skew):
    loads = [(1 << 20) // math.isqrt(standing ** skew) + 1 for standing in range(2, amount + 1)]
    surplus, given = total - bound - (amount - 1), [1] * (amount - 1)
    while surplus > 0:
        free = [i for i in range(amount - 1) if given[i] < bound]
        pool, budget = sum([loads[i] for i in free]), surplus
        for i in free:
            extra = min(bound - given[i], max(1, budget * loads[i] // pool), surplus)
            given[i] = given[i] + extra
            surplus = surplus - extra
    return np.array([bound] + given)


def ragged(stream_key, count, total, limit, lean):
    if count == 2:
        one = jax.random.randint(stream_key, (), max(1, total - limit), min(limit, total - 1) + 1)
        return jnp.stack([one, total - one])
    lengths = jnp.asarray(profile(count, total, limit, lean), jnp.int32)
    pairs = (count - 1) // 2
    donor, taker = lengths[1:1 + 2 * pairs:2], lengths[2:2 + 2 * pairs:2]
    margin = jnp.minimum(donor - 1, limit - taker)
    moved = jax.random.randint(jax.random.fold_in(stream_key, 1), (pairs,), 0, 1 << 20) % (margin + 1)
    lengths = lengths.at[1:1 + 2 * pairs:2].set(donor - moved).at[2:2 + 2 * pairs:2].set(taker + moved)
    return lengths[jax.random.permutation(jax.random.fold_in(stream_key, 2), count)]


def bell_draw(stream_key, dims, width, most, pieces=(), held_as=jnp.bfloat16):
    level = level_of(stream_key, dims, pieces, -0.22, 0.18) if pieces else 1.0
    drawn = jax.random.normal(stream_key, dims, jnp.float32) * width * level
    return jnp.minimum(jnp.maximum(drawn, -most), most).astype(held_as)


def setup_inputs(seed: int = 0) -> dict:
    key_of = jax.random.split(jax.random.key(seed), 3)
    return {
        "moments": bell_draw(key_of[0], (TENSORS, NB, BLK, D), 1.0, 6.0, ((2, 16), (3, 8)), jnp.float32),
        "owner_counts": ragged(key_of[1], N_ROW, NB, MOST, 2).astype(jnp.int32),
    }


def reference(moments, owner_counts):
    counts = owner_counts.astype(jnp.int32)
    starts = jnp.cumsum(counts) - counts
    slot_index = jnp.arange(MOST, dtype=jnp.int32)
    picked = starts[:, None] + slot_index[None, :]
    usable = slot_index[None, :] < counts[:, None]
    picked = jnp.where(usable, picked, 0).reshape(-1).astype(jnp.int32)
    usable_flat = usable.reshape(-1)

    def one_tensor(blocks):
        placed = jnp.where(usable_flat[:, None, None], jnp.take(blocks, picked, axis=0), jnp.zeros((), blocks.dtype))
        block_peak = jnp.max(jnp.abs(placed), axis=(1, 2))
        scale_value = jnp.maximum(block_peak, 1.0)
        scaled = (placed / scale_value[:, None, None]).reshape(-1, D)
        energy = jnp.sum(placed * placed, axis=(1, 2)) / (BLK * D)
        return scaled, scale_value, energy

    normalized, scales, energy = lax.map(one_tensor, moments)
    return normalized, scales, energy
```

```python
import functools
import jax
import jax.numpy as jnp
from jax import lax
from jax.sharding import PartitionSpec as P
from jax.experimental import pallas as pl
from jax.experimental.pallas import tpu as pltpu

SIDE = 4
HALF = 8
TIERS = (17, 18, 20, 22, 24, 32)
MESH = pl.DeviceIdType.MESH
TURNS = (1, 3, 2)


def plan_kernel(count_ref, plan_ref, tier_ref, col_ref, row_ref):
    for i in range(SIDE):
        col_ref[i] = 0
        row_ref[i] = 0
    groups = SIDE * SIDE
    start = jnp.int32(0)
    for g in range(groups):
        y, x = divmod(g, SIDE)
        n = count_ref[g]
        a = (n + (x + y) % 2) // 2
        plan_ref[0, g] = a
        plan_ref[1, g] = start
        plan_ref[4, g] = n
        col_ref[x] += a
        row_ref[y] += n - a
        start = start + n

    def improve(_, carry):
        for g in range(groups):
            y, x = divmod(g, SIDE)
            n = count_ref[g]
            a = plan_ref[0, g]
            gap = col_ref[x] - row_ref[y]
            step = jnp.where(gap >= 0, gap // 2, -((-gap) // 2))
            new = jnp.clip(a - step, jnp.maximum(n - HALF, 0), jnp.minimum(n, HALF))
            plan_ref[0, g] = new
            col_ref[x] += new - a
            row_ref[y] += a - new
        return carry

    lax.fori_loop(0, 3, improve, 0)
    need = jnp.int32(0)
    for i in range(SIDE):
        need = jnp.maximum(need, jnp.maximum(col_ref[i], row_ref[i]))
    tier = jnp.int32(0)
    for limit in TIERS[:-1]:
        tier = tier + (need > limit).astype(jnp.int32)
    tier_ref[0] = tier
    for x in range(SIDE):
        at = jnp.int32(0)
        for y in range(SIDE):
            g = y * SIDE + x
            plan_ref[2, g] = at
            at = at + plan_ref[0, g]
    for y in range(SIDE):
        at = jnp.int32(0)
        for x in range(SIDE):
            g = y * SIDE + x
            plan_ref[3, g] = at
            at = at + plan_ref[4, g] - plan_ref[0, g]


def move_kernel(
    slots, cols, plan_ref, moments_ref, x2_ref, y2_ref, stats_ref,
    mom0, mom1, send_x, send_y, got_x0, got_x1, got_y0, got_y1, out_x, out_y,
    pieces, stat_a, stat_b, stat_c, all_a, all_b, all_c,
    load_sem, send1, recv1, send2, recv2, own_sem, sa, ra, sb, rb,
):
    mom = (mom0, mom1)
    got_x = (got_x0, got_x1)
    got_y = (got_y0, got_y1)
    tensors = 2
    me = lax.axis_index("row")
    c = lax.axis_index("col")
    y, x = me // SIDE, me % SIDE
    blocks = mom0.shape[0]

    loads = [
        pltpu.make_async_copy(moments_ref.at[t], mom[t], load_sem.at[t])
        for t in range(tensors)
    ]
    for load in loads:
        load.start()

    def x_peer(d):
        return {"row": y * SIDE + (x + d) % SIDE}

    def y_peer(d):
        return {"row": ((y + d) % SIDE) * SIDE + x}

    barrier = pltpu.get_barrier_semaphore()
    for d in TURNS:
        pl.semaphore_signal(barrier, inc=1, device_id=x_peer(d), device_id_type=MESH)
        pl.semaphore_signal(barrier, inc=1, device_id=y_peer(d), device_id_type=MESH)
    for d in range(1, cols):
        pl.semaphore_signal(barrier, inc=1, device_id={"col": (c + d) % cols}, device_id_type=MESH)

    def order_x(xd):
        at = [plan_ref[2, i * SIDE + xd] for i in range(SIDE)]
        base = [plan_ref[1, i * SIDE + xd] - at[i] for i in range(SIDE)]

        def block_of(k):
            b = base[0]
            for i in range(1, SIDE):
                b = jnp.where(k >= at[i], base[i], b)
            return jnp.clip(b + k, 0, blocks - 1)

        return block_of

    def order_y(yd):
        at = [plan_ref[3, yd * SIDE + i] for i in range(SIDE)]
        base = [
            plan_ref[1, yd * SIDE + i] + plan_ref[0, yd * SIDE + i] - at[i]
            for i in range(SIDE)
        ]

        def block_of(k):
            b = base[0]
            for i in range(1, SIDE):
                b = jnp.where(k >= at[i], base[i], b)
            return jnp.clip(b + k, 0, blocks - 1)

        return block_of

    def pack1(t, block_of, dst):
        def step(k, carry):
            dst[k] = mom[t][block_of(k)]
            return carry

        lax.fori_loop(0, slots, step, 0, unroll=2)

    pl.semaphore_wait(barrier, 2 * (SIDE - 1) + cols - 1)

    first = [[], []]
    for t in range(tensors):
        loads[t].wait()
        for i, d in enumerate(TURNS):
            pack1(t, order_x((x + d) % SIDE), send_x.at[t, i])
            copy = pltpu.make_async_remote_copy(
                send_x.at[t, i], got_x[t].at[x], send1.at[t, 0, i], recv1.at[t, 0, i],
                device_id=x_peer(d), device_id_type=MESH)
            copy.start()
            first[t].append(copy)
            pack1(t, order_y((y + d) % SIDE), send_y.at[t, i])
            copy = pltpu.make_async_remote_copy(
                send_y.at[t, i], got_y[t].at[y], send1.at[t, 1, i], recv1.at[t, 1, i],
                device_id=y_peer(d), device_id_type=MESH)
            copy.start()
            first[t].append(copy)
        pack1(t, order_x(x), got_x[t].at[x])
        pack1(t, order_y(y), got_y[t].at[y])

    width = mom0.shape[2]
    for t in range(tensors):
        def measure(k, carry, t=t):
            rows = pl.ds(pl.multiple_of(k * 8, 8), 8)
            peak = None
            for w in range(0, width, 128):
                v = mom[t][rows, :, w:w + 128]
                m, q = jnp.abs(v), v * v
                peak, total = (m, q) if peak is None else (jnp.maximum(peak, m), total + q)
            pieces[t, rows, :] = jnp.max(peak, axis=1)
            pieces[2 + t, rows, :] = jnp.sum(total, axis=1)
            return carry

        lax.fori_loop(0, blocks // 8, measure, 0)
    stat_a[...] = jnp.zeros_like(stat_a)
    for t in range(tensors):
        stat_a[t:t + 1, :] = jnp.max(pieces[t].T, axis=0, keepdims=True)
        stat_a[2 + t:3 + t, :] = jnp.sum(pieces[2 + t].T, axis=0, keepdims=True)
    is_peak = lax.broadcasted_iota(jnp.int32, stat_a.shape, 0) < tensors

    def join(mine, others, n):
        v = mine[...]
        for i in range(n):
            o = others[i]
            v = jnp.where(is_peak, jnp.maximum(v, o), v + o)
        return v

    stage = []
    for d in range(1, cols):
        copy = pltpu.make_async_remote_copy(
            stat_a, all_a.at[d - 1], sa.at[d - 1], ra.at[d - 1],
            device_id={"col": (c + d) % cols}, device_id_type=MESH)
        copy.start()
        stage.append(copy)
    for copy in stage:
        copy.wait()
    stat_b[...] = join(stat_a, all_a, cols - 1)
    stage = []
    for i, d in enumerate(TURNS):
        copy = pltpu.make_async_remote_copy(
            stat_b, all_b.at[i], sb.at[0, i], rb.at[0, i],
            device_id=x_peer(d), device_id_type=MESH)
        copy.start()
        stage.append(copy)

    def pack2(got, offset, dst):
        def step(j, carry):
            k = jnp.minimum(offset + j, slots - 1)
            for s in range(SIDE):
                dst[j, s] = got[s, k]
            return carry

        lax.fori_loop(0, HALF, step, 0)

    second = []
    own = []
    for t in range(tensors):
        for copy in first[t]:
            copy.wait_recv()
        if t == 1:
            for copy in stage:
                copy.wait()
            stat_c[...] = join(stat_b, all_b, SIDE - 1)
            stage = []
            for i, d in enumerate(TURNS):
                copy = pltpu.make_async_remote_copy(
                    stat_c, all_c.at[i], sb.at[1, i], rb.at[1, i],
                    device_id=y_peer(d), device_id_type=MESH)
                copy.start()
                stage.append(copy)
        for i, d in enumerate(TURNS):
            yd, xd = (y + d) % SIDE, (x + d) % SIDE
            pack2(got_x[t], plan_ref[2, yd * SIDE + x], out_x.at[t, i])
            copy = pltpu.make_async_remote_copy(
                out_x.at[t, i], x2_ref.at[y, t], send2.at[t, 0, i], recv2.at[t, 0, i],
                device_id=y_peer(d), device_id_type=MESH)
            copy.start()
            second.append(copy)
            pack2(got_y[t], plan_ref[3, y * SIDE + xd], out_y.at[t, i])
            copy = pltpu.make_async_remote_copy(
                out_y.at[t, i], y2_ref.at[x, t], send2.at[t, 1, i], recv2.at[t, 1, i],
                device_id=x_peer(d), device_id_type=MESH)
            copy.start()
            second.append(copy)
        pack2(got_x[t], plan_ref[2, me], out_x.at[t, 3])
        copy = pltpu.make_async_copy(out_x.at[t, 3], x2_ref.at[y, t], own_sem.at[t, 0])
        copy.start()
        own.append(copy)
        pack2(got_y[t], plan_ref[3, me], out_y.at[t, 3])
        copy = pltpu.make_async_copy(out_y.at[t, 3], y2_ref.at[x, t], own_sem.at[t, 1])
        copy.start()
        own.append(copy)

    for t in range(tensors):
        for copy in first[t]:
            copy.wait_send()
    for copy in stage:
        copy.wait()
    stats_ref[...] = join(stat_c, all_c, SIDE - 1)
    for copy in own:
        copy.wait()
    for copy in second:
        copy.wait()


def place_kernel(
    full_size, plan_ref, stats_ref, x2_ref, y2_ref, norm_ref, scale_ref, energy_ref,
    inb, outb, zeros, in_sem, out_sem,
):
    tensors, capacity = scale_ref.shape
    me = lax.axis_index("row")
    a, start, n = plan_ref[0, me], plan_ref[1, me], plan_ref[4, me]
    zeros[...] = jnp.zeros_like(zeros)
    rows = zeros.shape[0]

    def out_rows(j):
        return pl.ds(pl.multiple_of(j * rows, rows), rows)

    def put(t, j, src):
        return pltpu.make_async_copy(src, norm_ref.at[t, out_rows(j)], out_sem.at[t, j])

    def take_x(t, j):
        return pltpu.make_async_copy(x2_ref.at[:, t, j], inb.at[t, j], in_sem.at[t, j])

    def take_y(t, j):
        return pltpu.make_async_copy(y2_ref.at[:, t, j - a], inb.at[t, j], in_sem.at[t, j])

    for t in range(tensors):
        lax.fori_loop(0, a, lambda j, _: (take_x(t, j).start(), _)[1], 0)
        lax.fori_loop(a, n, lambda j, _: (take_y(t, j).start(), _)[1], 0)
    for t in range(tensors):
        lax.fori_loop(n, capacity, lambda j, _: (put(t, j, zeros).start(), _)[1], 0)

    for t in range(tensors):
        def scale_of(j, t=t):
            return jnp.maximum(stats_ref[t, start + j], 1.0)

        def inverse(j):
            return 1.0 / jnp.full((8, 128), scale_of(j), jnp.float32)

        def scaled(j, carry, t=t, swap=False, take=take_x):
            take(t, j).wait()
            inv = inverse(j)[:, :1]
            for p in range(SIDE):
                for q in range(SIDE):
                    r = (q * SIDE + p) if swap else (p * SIDE + q)
                    outb[t, j, r * 8:r * 8 + 8, :] = inb[t, j, p, q] * inv
            put(t, j, outb.at[t, j]).start()
            return carry

        lax.fori_loop(0, a, functools.partial(scaled, swap=False, take=take_x), 0)
        lax.fori_loop(a, n, functools.partial(scaled, swap=True, take=take_y), 0)
        for j in range(capacity):
            used = j < n
            at = jnp.minimum(start + j, stats_ref.shape[1] - 1)
            scale_ref[t, j] = jnp.where(used, jnp.maximum(stats_ref[t, at], 1.0), 1.0)
            energy_ref[t, j] = jnp.where(used, stats_ref[tensors + t, at] / full_size, 0.0)
    for t in range(tensors):
        lax.fori_loop(0, capacity, lambda j, _: (put(t, j, zeros).wait(), _)[1], 0)


def on_device(moments, owner_counts):
    tensors, blocks, sub, width = moments.shape
    groups, cols = lax.axis_size("row"), lax.axis_size("col")
    capacity = 2 * HALF
    f32, i32 = jnp.float32, jnp.int32
    smem = pl.BlockSpec(memory_space=pltpu.SMEM)
    hbm = pl.BlockSpec(memory_space=pl.ANY)
    vmem = pl.BlockSpec(memory_space=pltpu.VMEM)

    plan, tier = pl.pallas_call(
        plan_kernel,
        out_shape=(jax.ShapeDtypeStruct((8, groups), i32), jax.ShapeDtypeStruct((1,), i32)),
        in_specs=[smem],
        out_specs=(smem, smem),
        scratch_shapes=[pltpu.SMEM((SIDE,), i32), pltpu.SMEM((SIDE,), i32)],
        name="plan",
    )(owner_counts)

    def branch(number, slots):
        arrived = jax.ShapeDtypeStruct((SIDE, tensors, HALF, SIDE, sub, width), f32)
        got = pltpu.VMEM((SIDE, slots, sub, width), f32)
        sent = pltpu.VMEM((tensors, SIDE - 1, slots, sub, width), f32)
        out = pltpu.VMEM((tensors, SIDE, HALF, SIDE, sub, width), f32)
        stat = pltpu.VMEM((8, blocks), f32)
        dma = pltpu.SemaphoreType.DMA
        peers = max(cols - 1, 1)

        def run(moments, plan):
            x2, y2, stats = pl.pallas_call(
                functools.partial(move_kernel, slots, cols),
                out_shape=(arrived, arrived, jax.ShapeDtypeStruct((8, blocks), f32)),
                in_specs=[smem, hbm],
                out_specs=(hbm, hbm, vmem),
                scratch_shapes=[
                    pltpu.VMEM((blocks, sub, width), f32), pltpu.VMEM((blocks, sub, width), f32),
                    sent, sent, got, got, got, got, out, out,
                    pltpu.VMEM((4, blocks, 128), f32), stat, stat, stat,
                    pltpu.VMEM((peers, 8, blocks), f32),
                    pltpu.VMEM((SIDE - 1, 8, blocks), f32),
                    pltpu.VMEM((SIDE - 1, 8, blocks), f32),
                    dma((2,)), dma((2, 2, 3)), dma((2, 2, 3)), dma((2, 2, 3)), dma((2, 2, 3)),
                    dma((2, 2)), dma((peers,)), dma((peers,)), dma((2, 3)), dma((2, 3)),
                ],
                compiler_params=pltpu.CompilerParams(
                    collective_id=number, has_side_effects=True, vmem_limit_bytes=56 * 2**20),
                name=f"move{slots}",
            )(plan, moments)
            return pl.pallas_call(
                functools.partial(place_kernel, float(sub * groups * width * cols)),
                out_shape=(
                    jax.ShapeDtypeStruct((tensors, capacity * sub * groups, width), f32),
                    jax.ShapeDtypeStruct((tensors, capacity), f32),
                    jax.ShapeDtypeStruct((tensors, capacity), f32),
                ),
                in_specs=[smem, smem, hbm, hbm],
                out_specs=(hbm, smem, smem),
                scratch_shapes=[
                    pltpu.VMEM((tensors, capacity, SIDE, SIDE, sub, width), f32),
                    pltpu.VMEM((tensors, capacity, sub * groups, width), f32),
                    pltpu.VMEM((sub * groups, width), f32),
                    dma((tensors, capacity)), dma((tensors, capacity)),
                ],
                compiler_params=pltpu.CompilerParams(vmem_limit_bytes=40 * 2**20),
                name="place",
            )(plan, stats, x2, y2)

        return run

    return lax.switch(tier[0], [branch(i, s) for i, s in enumerate(TIERS)], moments, plan)


def solution(mesh):
    placed = (P(None, None, "row", "col"), P())
    return jax.shard_map(
        on_device,
        mesh=mesh,
        in_specs=placed,
        out_specs=(P(None, "row", "col"), P(None, "row"), P(None, "row")),
        check_vma=False,
    )
```

```python
import functools
import jax
import jax.numpy as jnp
from jax import lax
from jax.sharding import PartitionSpec as P
from jax.experimental import pallas as pl
from jax.experimental.pallas import tpu as pltpu

SIDE = 4
HALF = 8
TIERS = (17, 18, 20, 22, 24, 32)
MESH = pl.DeviceIdType.MESH
TURNS = (1, 3, 2)


def plan_kernel(count_ref, plan_ref, tier_ref, col_ref, row_ref):
    for i in range(SIDE):
        col_ref[i] = 0
        row_ref[i] = 0
    groups = SIDE * SIDE
    start = jnp.int32(0)
    for g in range(groups):
        y, x = divmod(g, SIDE)
        n = count_ref[g]
        a = (n + (x + y) % 2) // 2
        plan_ref[0, g] = a
        plan_ref[1, g] = start
        plan_ref[4, g] = n
        col_ref[x] += a
        row_ref[y] += n - a
        start = start + n

    def improve(_, carry):
        for g in range(groups):
            y, x = divmod(g, SIDE)
            n = count_ref[g]
            a = plan_ref[0, g]
            gap = col_ref[x] - row_ref[y]
            step = jnp.where(gap >= 0, gap // 2, -((-gap) // 2))
            new = jnp.clip(a - step, jnp.maximum(n - HALF, 0), jnp.minimum(n, HALF))
            plan_ref[0, g] = new
            col_ref[x] += new - a
            row_ref[y] += a - new
        return carry

    lax.fori_loop(0, 3, improve, 0)
    need = jnp.int32(0)
    for i in range(SIDE):
        need = jnp.maximum(need, jnp.maximum(col_ref[i], row_ref[i]))
    tier = jnp.int32(0)
    for limit in TIERS[:-1]:
        tier = tier + (need > limit).astype(jnp.int32)
    tier_ref[0] = tier
    for x in range(SIDE):
        at = jnp.int32(0)
        for y in range(SIDE):
            g = y * SIDE + x
            plan_ref[2, g] = at
            at = at + plan_ref[0, g]
    for y in range(SIDE):
        at = jnp.int32(0)
        for x in range(SIDE):
            g = y * SIDE + x
            plan_ref[3, g] = at
            at = at + plan_ref[4, g] - plan_ref[0, g]


def move_kernel(
    slots, cols, plan_ref, moments_ref, x2_ref, y2_ref, stats_ref,
    mom0, mom1, send_x, send_y, got_x0, got_x1, got_y0, got_y1, out_x, out_y,
    pieces, stat_a, stat_b, stat_c, all_a, all_b, all_c,
    load_sem, send1, recv1, send2, recv2, sa, ra, sb, rb,
):
    mom = (mom0, mom1)
    got_x = (got_x0, got_x1)
    got_y = (got_y0, got_y1)
    tensors = 2
    me = lax.axis_index("row")
    c = lax.axis_index("col")
    y, x = me // SIDE, me % SIDE
    blocks = mom0.shape[0]

    loads = [
        pltpu.make_async_copy(moments_ref.at[t], mom[t], load_sem.at[t])
        for t in range(tensors)
    ]
    for load in loads:
        load.start()

    def x_peer(d):
        return {"row": y * SIDE + (x + d) % SIDE}

    def y_peer(d):
        return {"row": ((y + d) % SIDE) * SIDE + x}

    barrier = pltpu.get_barrier_semaphore()
    for d in TURNS:
        pl.semaphore_signal(barrier, inc=1, device_id=x_peer(d), device_id_type=MESH)
        pl.semaphore_signal(barrier, inc=1, device_id=y_peer(d), device_id_type=MESH)
    for d in range(1, cols):
        pl.semaphore_signal(barrier, inc=1, device_id={"col": (c + d) % cols}, device_id_type=MESH)

    def order_x(xd):
        at = [plan_ref[2, i * SIDE + xd] for i in range(SIDE)]
        base = [plan_ref[1, i * SIDE + xd] - at[i] for i in range(SIDE)]

        def block_of(k):
            b = base[0]
            for i in range(1, SIDE):
                b = jnp.where(k >= at[i], base[i], b)
            return jnp.clip(b + k, 0, blocks - 1)

        return block_of

    def order_y(yd):
        at = [plan_ref[3, yd * SIDE + i] for i in range(SIDE)]
        base = [
            plan_ref[1, yd * SIDE + i] + plan_ref[0, yd * SIDE + i] - at[i]
            for i in range(SIDE)
        ]

        def block_of(k):
            b = base[0]
            for i in range(1, SIDE):
                b = jnp.where(k >= at[i], base[i], b)
            return jnp.clip(b + k, 0, blocks - 1)

        return block_of

    def pack1(t, block_of, dst):
        def step(k, carry):
            dst[k] = mom[t][block_of(k)]
            return carry

        lax.fori_loop(0, slots, step, 0, unroll=2)

    pl.semaphore_wait(barrier, 2 * (SIDE - 1) + cols - 1)

    first = [[], []]
    for t in range(tensors):
        loads[t].wait()
        for i, d in enumerate(TURNS):
            pack1(t, order_x((x + d) % SIDE), send_x.at[t, i])
            copy = pltpu.make_async_remote_copy(
                send_x.at[t, i], got_x[t].at[x], send1.at[t, 0, i], recv1.at[t, 0, i],
                device_id=x_peer(d), device_id_type=MESH)
            copy.start()
            first[t].append(copy)
            pack1(t, order_y((y + d) % SIDE), send_y.at[t, i])
            copy = pltpu.make_async_remote_copy(
                send_y.at[t, i], got_y[t].at[y], send1.at[t, 1, i], recv1.at[t, 1, i],
                device_id=y_peer(d), device_id_type=MESH)
            copy.start()
            first[t].append(copy)
        pack1(t, order_x(x), got_x[t].at[x])
        pack1(t, order_y(y), got_y[t].at[y])

    width = mom0.shape[2]
    for t in range(tensors):
        def measure(k, carry, t=t):
            rows = pl.ds(pl.multiple_of(k * 8, 8), 8)
            peak = None
            for w in range(0, width, 128):
                v = mom[t][rows, :, w:w + 128]
                m, q = jnp.abs(v), v * v
                peak, total = (m, q) if peak is None else (jnp.maximum(peak, m), total + q)
            pieces[t, rows, :] = jnp.max(peak, axis=1)
            pieces[2 + t, rows, :] = jnp.sum(total, axis=1)
            return carry

        lax.fori_loop(0, blocks // 8, measure, 0)
    stat_a[...] = jnp.zeros_like(stat_a)
    for t in range(tensors):
        stat_a[t:t + 1, :] = jnp.max(pieces[t].T, axis=0, keepdims=True)
        stat_a[2 + t:3 + t, :] = jnp.sum(pieces[2 + t].T, axis=0, keepdims=True)
    is_peak = lax.broadcasted_iota(jnp.int32, stat_a.shape, 0) < tensors

    def join(mine, others, n):
        v = mine[...]
        for i in range(n):
            o = others[i]
            v = jnp.where(is_peak, jnp.maximum(v, o), v + o)
        return v

    stage = []
    for d in range(1, cols):
        copy = pltpu.make_async_remote_copy(
            stat_a, all_a.at[d - 1], sa.at[d - 1], ra.at[d - 1],
            device_id={"col": (c + d) % cols}, device_id_type=MESH)
        copy.start()
        stage.append(copy)
    for copy in stage:
        copy.wait()
    stat_b[...] = join(stat_a, all_a, cols - 1)
    stage = []
    for i, d in enumerate(TURNS):
        copy = pltpu.make_async_remote_copy(
            stat_b, all_b.at[i], sb.at[0, i], rb.at[0, i],
            device_id=x_peer(d), device_id_type=MESH)
        copy.start()
        stage.append(copy)

    def pack2(got, offset, dst):
        def step(j, carry):
            k = jnp.minimum(offset + j, slots - 1)
            for s in range(SIDE):
                dst[j, s] = got[s, k]
            return carry

        lax.fori_loop(0, HALF, step, 0)

    second = []
    for t in range(tensors):
        for copy in first[t]:
            copy.wait_recv()
        if t == 1:
            for copy in stage:
                copy.wait()
            stat_c[...] = join(stat_b, all_b, SIDE - 1)
            stage = []
            for i, d in enumerate(TURNS):
                copy = pltpu.make_async_remote_copy(
                    stat_c, all_c.at[i], sb.at[1, i], rb.at[1, i],
                    device_id=y_peer(d), device_id_type=MESH)
                copy.start()
                stage.append(copy)
        for i, d in enumerate(TURNS):
            yd, xd = (y + d) % SIDE, (x + d) % SIDE
            pack2(got_x[t], plan_ref[2, yd * SIDE + x], out_x.at[t, i])
            copy = pltpu.make_async_remote_copy(
                out_x.at[t, i], x2_ref.at[y, t], send2.at[t, 0, i], recv2.at[t, 0, i],
                device_id=y_peer(d), device_id_type=MESH)
            copy.start()
            second.append(copy)
            pack2(got_y[t], plan_ref[3, y * SIDE + xd], out_y.at[t, i])
            copy = pltpu.make_async_remote_copy(
                out_y.at[t, i], y2_ref.at[x, t], send2.at[t, 1, i], recv2.at[t, 1, i],
                device_id=x_peer(d), device_id_type=MESH)
            copy.start()
            second.append(copy)
        pack2(got_x[t], plan_ref[2, me], x2_ref.at[y, t])
        pack2(got_y[t], plan_ref[3, me], y2_ref.at[x, t])

    for t in range(tensors):
        for copy in first[t]:
            copy.wait_send()
    for copy in stage:
        copy.wait()
    stats_ref[...] = join(stat_c, all_c, SIDE - 1)
    for copy in second:
        copy.wait()


def place_kernel(
    full_size, plan_ref, stats_ref, x2_ref, y2_ref, norm_ref, scale_ref, energy_ref,
    outb, zeros, out_sem,
):
    tensors, capacity = scale_ref.shape
    me = lax.axis_index("row")
    a, start, n = plan_ref[0, me], plan_ref[1, me], plan_ref[4, me]
    zeros[...] = jnp.zeros_like(zeros)
    rows = zeros.shape[0]

    def put(t, j, src):
        at = pl.ds(pl.multiple_of(j * rows, rows), rows)
        return pltpu.make_async_copy(src, norm_ref.at[t, at], out_sem.at[t, j])

    for t in range(tensors):
        lax.fori_loop(n, capacity, lambda j, _: (put(t, j, zeros).start(), _)[1], 0)

    for t in range(tensors):
        def scaled(j, carry, t=t, swap=False):
            scale = jnp.maximum(stats_ref[t, start + j], 1.0)
            inv = (1.0 / jnp.full((8, 128), scale, jnp.float32))[:, :1]
            for p in range(SIDE):
                for q in range(SIDE):
                    r = (q * SIDE + p) if swap else (p * SIDE + q)
                    part = y2_ref[p, t, j - a, q] if swap else x2_ref[p, t, j, q]
                    outb[t, j, r * 8:r * 8 + 8, :] = part * inv
            put(t, j, outb.at[t, j]).start()
            return carry

        lax.fori_loop(0, a, functools.partial(scaled, swap=False), 0)
        lax.fori_loop(a, n, functools.partial(scaled, swap=True), 0)
        for j in range(capacity):
            used = j < n
            at = jnp.minimum(start + j, stats_ref.shape[1] - 1)
            scale_ref[t, j] = jnp.where(used, jnp.maximum(stats_ref[t, at], 1.0), 1.0)
            energy_ref[t, j] = jnp.where(used, stats_ref[tensors + t, at] / full_size, 0.0)
    for t in range(tensors):
        lax.fori_loop(0, capacity, lambda j, _: (put(t, j, zeros).wait(), _)[1], 0)


def on_device(moments, owner_counts):
    tensors, blocks, sub, width = moments.shape
    groups, cols = lax.axis_size("row"), lax.axis_size("col")
    capacity = 2 * HALF
    f32, i32 = jnp.float32, jnp.int32
    smem = pl.BlockSpec(memory_space=pltpu.SMEM)
    hbm = pl.BlockSpec(memory_space=pl.ANY)
    vmem = pl.BlockSpec(memory_space=pltpu.VMEM)

    plan, tier = pl.pallas_call(
        plan_kernel,
        out_shape=(jax.ShapeDtypeStruct((8, groups), i32), jax.ShapeDtypeStruct((1,), i32)),
        in_specs=[smem],
        out_specs=(smem, smem),
        scratch_shapes=[pltpu.SMEM((SIDE,), i32), pltpu.SMEM((SIDE,), i32)],
        name="plan",
    )(owner_counts)

    def branch(number, slots):
        arrived = pltpu.VMEM((SIDE, tensors, HALF, SIDE, sub, width), f32)
        got = pltpu.VMEM((SIDE, slots, sub, width), f32)
        sent = pltpu.VMEM((tensors, SIDE - 1, slots, sub, width), f32)
        out = pltpu.VMEM((tensors, SIDE - 1, HALF, SIDE, sub, width), f32)
        stat = pltpu.VMEM((8, blocks), f32)
        dma = pltpu.SemaphoreType.DMA
        peers = max(cols - 1, 1)
        piece = 4 * sub * width
        limit = piece * (2 * blocks + 28 * slots + 48 * HALF) + 1 * 2**20

        def run(moments, plan):
            x2, y2, stats = pl.pallas_call(
                functools.partial(move_kernel, slots, cols),
                out_shape=(arrived, arrived, jax.ShapeDtypeStruct((8, blocks), f32)),
                in_specs=[smem, hbm],
                out_specs=(vmem, vmem, vmem),
                scratch_shapes=[
                    pltpu.VMEM((blocks, sub, width), f32), pltpu.VMEM((blocks, sub, width), f32),
                    sent, sent, got, got, got, got, out, out,
                    pltpu.VMEM((4, blocks, 128), f32), stat, stat, stat,
                    pltpu.VMEM((peers, 8, blocks), f32),
                    pltpu.VMEM((SIDE - 1, 8, blocks), f32),
                    pltpu.VMEM((SIDE - 1, 8, blocks), f32),
                    dma((2,)), dma((2, 2, 3)), dma((2, 2, 3)), dma((2, 2, 3)), dma((2, 2, 3)),
                    dma((peers,)), dma((peers,)), dma((2, 3)), dma((2, 3)),
                ],
                compiler_params=pltpu.CompilerParams(
                    collective_id=number, has_side_effects=True, vmem_limit_bytes=limit),
                name=f"move{slots}",
            )(plan, moments)
            return pl.pallas_call(
                functools.partial(place_kernel, float(sub * groups * width * cols)),
                out_shape=(
                    jax.ShapeDtypeStruct((tensors, capacity * sub * groups, width), f32),
                    jax.ShapeDtypeStruct((tensors, capacity), f32),
                    jax.ShapeDtypeStruct((tensors, capacity), f32),
                ),
                in_specs=[smem, smem, vmem, vmem],
                out_specs=(hbm, smem, smem),
                scratch_shapes=[
                    pltpu.VMEM((tensors, capacity, sub * groups, width), f32),
                    pltpu.VMEM((sub * groups, width), f32),
                    dma((tensors, capacity)),
                ],
                compiler_params=pltpu.CompilerParams(vmem_limit_bytes=16 * 2**20),
                name="place",
            )(plan, stats, x2, y2)

        return run

    return lax.switch(tier[0], [branch(i, s) for i, s in enumerate(TIERS)], moments, plan)


def solution(mesh):
    placed = (P(None, None, "row", "col"), P())
    return jax.shard_map(
        on_device,
        mesh=mesh,
        in_specs=placed,
        out_specs=(P(None, "row", "col"), P(None, "row"), P(None, "row")),
        check_vma=False,
    )
```

```python
import functools
import jax
import jax.numpy as jnp
from jax import lax
from jax.sharding import PartitionSpec as P
from jax.experimental import pallas as pl
from jax.experimental.pallas import tpu as pltpu

SIDE = 4
GROUPS = SIDE * SIDE
HALF = 8
TIERS = (17, 18, 19, 20, 21, 22, 23, 24, 26, 28, 32)
MESH = pl.DeviceIdType.MESH
TURNS = (1, 3, 2)


def plan_kernel(count_ref, plan_ref, tier_ref):
    groups = SIDE * SIDE
    n = [count_ref[g] for g in range(groups)]
    low = [jnp.maximum(v - HALF, 0) for v in n]
    high = [jnp.minimum(v, HALF) for v in n]
    a = [(n[g] + (g // SIDE + g % SIDE) % 2) // 2 for g in range(groups)]
    col = [sum(a[x::SIDE]) for x in range(SIDE)]
    row = [sum(n[y * SIDE:(y + 1) * SIDE]) - sum(a[y * SIDE:(y + 1) * SIDE]) for y in range(SIDE)]
    for _ in range(2):
        for g in range(groups):
            y, x = divmod(g, SIDE)
            new = jnp.clip(a[g] - ((col[x] - row[y] + 1) >> 1), low[g], high[g])
            col[x] = col[x] + new - a[g]
            row[y] = row[y] + a[g] - new
            a[g] = new
    need = functools.reduce(jnp.maximum, col + row)
    tier = jnp.int32(0)
    for limit in TIERS[:-1]:
        tier = tier + (need > limit).astype(jnp.int32)
    tier_ref[0] = tier
    start = jnp.int32(0)
    at_x, at_y = [jnp.int32(0)] * SIDE, [jnp.int32(0)] * SIDE
    for g in range(groups):
        y, x = divmod(g, SIDE)
        plan_ref[g] = a[g]
        plan_ref[groups + g] = start
        plan_ref[2 * groups + g] = at_x[x]
        plan_ref[3 * groups + g] = at_y[y]
        plan_ref[4 * groups + g] = n[g]
        start = start + n[g]
        at_x[x] = at_x[x] + a[g]
        at_y[y] = at_y[y] + n[g] - a[g]


def move_kernel(
    slots, cols, plan_in, moments_ref, x2_ref, y2_ref, stats_ref,
    mom0, mom1, send_x, send_y, got_x0, got_x1, got_y0, got_y1, out_x, out_y,
    pieces, stat_a, stat_b, stat_c, all_a, all_b, all_c,
    plan_ref, plan_sem, load_sem, send1, recv1, send2, recv2, sa, ra, sb, rb,
):
    mom = (mom0, mom1)
    got_x = (got_x0, got_x1)
    got_y = (got_y0, got_y1)
    tensors = 2
    me = lax.axis_index("row")
    c = lax.axis_index("col")
    y, x = me // SIDE, me % SIDE
    blocks = mom0.shape[0]

    loads = [
        pltpu.make_async_copy(moments_ref.at[t], mom[t], load_sem.at[t])
        for t in range(tensors)
    ]
    table = pltpu.make_async_copy(plan_in, plan_ref, plan_sem)
    table.start()
    for load in loads:
        load.start()

    def x_peer(d):
        return {"row": y * SIDE + (x + d) % SIDE}

    def y_peer(d):
        return {"row": ((y + d) % SIDE) * SIDE + x}

    barrier = pltpu.get_barrier_semaphore()
    for d in TURNS:
        pl.semaphore_signal(barrier, inc=1, device_id=x_peer(d), device_id_type=MESH)
        pl.semaphore_signal(barrier, inc=1, device_id=y_peer(d), device_id_type=MESH)
    for d in range(1, cols):
        pl.semaphore_signal(barrier, inc=1, device_id={"col": (c + d) % cols}, device_id_type=MESH)

    def order_x(xd):
        at = [plan_ref[2 * GROUPS + i * SIDE + xd] for i in range(SIDE)]
        base = [plan_ref[GROUPS + i * SIDE + xd] - at[i] for i in range(SIDE)]

        def block_of(k):
            b = base[0]
            for i in range(1, SIDE):
                b = jnp.where(k >= at[i], base[i], b)
            return jnp.clip(b + k, 0, blocks - 1)

        return block_of

    def order_y(yd):
        at = [plan_ref[3 * GROUPS + yd * SIDE + i] for i in range(SIDE)]
        base = [
            plan_ref[GROUPS + yd * SIDE + i] + plan_ref[yd * SIDE + i] - at[i]
            for i in range(SIDE)
        ]

        def block_of(k):
            b = base[0]
            for i in range(1, SIDE):
                b = jnp.where(k >= at[i], base[i], b)
            return jnp.clip(b + k, 0, blocks - 1)

        return block_of

    def pack1(t, block_of, dst):
        def step(k, carry):
            dst[k] = mom[t][block_of(k)]
            return carry

        lax.fori_loop(0, slots, step, 0, unroll=2)

    table.wait()
    pl.semaphore_wait(barrier, 2 * (SIDE - 1) + cols - 1)

    first = [[], []]
    for t in range(tensors):
        loads[t].wait()
        for i, d in enumerate(TURNS):
            pack1(t, order_x((x + d) % SIDE), send_x.at[t, i])
            copy = pltpu.make_async_remote_copy(
                send_x.at[t, i], got_x[t].at[x], send1.at[t, 0, i], recv1.at[t, 0, i],
                device_id=x_peer(d), device_id_type=MESH)
            copy.start()
            first[t].append(copy)
            pack1(t, order_y((y + d) % SIDE), send_y.at[t, i])
            copy = pltpu.make_async_remote_copy(
                send_y.at[t, i], got_y[t].at[y], send1.at[t, 1, i], recv1.at[t, 1, i],
                device_id=y_peer(d), device_id_type=MESH)
            copy.start()
            first[t].append(copy)
        pack1(t, order_x(x), got_x[t].at[x])
        pack1(t, order_y(y), got_y[t].at[y])

    width = mom0.shape[2]
    for t in range(tensors):
        def measure(k, carry, t=t):
            rows = pl.ds(pl.multiple_of(k * 8, 8), 8)
            peak = None
            for w in range(0, width, 128):
                v = mom[t][rows, :, w:w + 128]
                m, q = jnp.abs(v), v * v
                peak, total = (m, q) if peak is None else (jnp.maximum(peak, m), total + q)
            pieces[t, rows, :] = jnp.max(peak, axis=1)
            pieces[2 + t, rows, :] = jnp.sum(total, axis=1)
            return carry

        lax.fori_loop(0, blocks // 8, measure, 0)
    stat_a[...] = jnp.zeros_like(stat_a)
    for t in range(tensors):
        stat_a[t:t + 1, :] = jnp.max(pieces[t].T, axis=0, keepdims=True)
        stat_a[2 + t:3 + t, :] = jnp.sum(pieces[2 + t].T, axis=0, keepdims=True)
    is_peak = lax.broadcasted_iota(jnp.int32, stat_a.shape, 0) < tensors

    def join(mine, others, n):
        v = mine[...]
        for i in range(n):
            o = others[i]
            v = jnp.where(is_peak, jnp.maximum(v, o), v + o)
        return v

    stage = []
    for d in range(1, cols):
        copy = pltpu.make_async_remote_copy(
            stat_a, all_a.at[d - 1], sa.at[d - 1], ra.at[d - 1],
            device_id={"col": (c + d) % cols}, device_id_type=MESH)
        copy.start()
        stage.append(copy)
    for copy in stage:
        copy.wait()
    stat_b[...] = join(stat_a, all_a, cols - 1)
    stage = []
    for i, d in enumerate(TURNS):
        copy = pltpu.make_async_remote_copy(
            stat_b, all_b.at[i], sb.at[0, i], rb.at[0, i],
            device_id=x_peer(d), device_id_type=MESH)
        copy.start()
        stage.append(copy)

    def pack2(got, offset, dst):
        def step(j, carry):
            k = jnp.minimum(offset + j, slots - 1)
            for s in range(SIDE):
                dst[j, s] = got[s, k]
            return carry

        lax.fori_loop(0, HALF, step, 0)

    second = []
    for t in range(tensors):
        for copy in first[t]:
            copy.wait_recv()
        if t == 1:
            for copy in stage:
                copy.wait()
            stat_c[...] = join(stat_b, all_b, SIDE - 1)
            stage = []
            for i, d in enumerate(TURNS):
                copy = pltpu.make_async_remote_copy(
                    stat_c, all_c.at[i], sb.at[1, i], rb.at[1, i],
                    device_id=y_peer(d), device_id_type=MESH)
                copy.start()
                stage.append(copy)
        for i, d in enumerate(TURNS):
            yd, xd = (y + d) % SIDE, (x + d) % SIDE
            pack2(got_x[t], plan_ref[2 * GROUPS + yd * SIDE + x], out_x.at[t, i])
            copy = pltpu.make_async_remote_copy(
                out_x.at[t, i], x2_ref.at[y, t], send2.at[t, 0, i], recv2.at[t, 0, i],
                device_id=y_peer(d), device_id_type=MESH)
            copy.start()
            second.append(copy)
            pack2(got_y[t], plan_ref[3 * GROUPS + y * SIDE + xd], out_y.at[t, i])
            copy = pltpu.make_async_remote_copy(
                out_y.at[t, i], y2_ref.at[x, t], send2.at[t, 1, i], recv2.at[t, 1, i],
                device_id=x_peer(d), device_id_type=MESH)
            copy.start()
            second.append(copy)
        pack2(got_x[t], plan_ref[2 * GROUPS + me], x2_ref.at[y, t])
        pack2(got_y[t], plan_ref[3 * GROUPS + me], y2_ref.at[x, t])

    for t in range(tensors):
        for copy in first[t]:
            copy.wait_send()
    for copy in stage:
        copy.wait()
    stats_ref[...] = join(stat_c, all_c, SIDE - 1)
    for copy in second:
        copy.wait()


def place_kernel(
    full_size, plan_ref, stats_ref, x2_ref, y2_ref, norm_ref, scale_out, energy_out,
    outb, zeros, inverse, scale_ref, energy_ref, out_sem, small_sem,
):
    tensors, capacity = scale_ref.shape
    me = lax.axis_index("row")
    a, start, n = plan_ref[me], plan_ref[GROUPS + me], plan_ref[4 * GROUPS + me]
    zeros[...] = jnp.zeros_like(zeros)
    rows = zeros.shape[0]

    def put(t, j, src):
        at = pl.ds(pl.multiple_of(j * rows, rows), rows)
        return pltpu.make_async_copy(src, norm_ref.at[t, at], out_sem.at[t, j])

    for t in range(tensors):
        lax.fori_loop(n, capacity, lambda j, _: (put(t, j, zeros).start(), _)[1], 0)

    lanes = stats_ref.shape[1]
    mine = pltpu.roll(stats_ref[...], lax.rem(lanes - start, lanes), 1)
    lane = lax.broadcasted_iota(jnp.int32, mine.shape, 1)
    scale = jnp.where(lane < n, jnp.maximum(mine, 1.0), 1.0)
    energy = jnp.where(lane < n, mine / full_size, 0.0)
    scale_ref[...] = scale[:tensors, :capacity]
    energy_ref[...] = energy[tensors:2 * tensors, :capacity]
    inv = 1.0 / scale
    pick = lax.broadcasted_iota(jnp.int32, (capacity, lanes), 0)
    pick = pick == lax.broadcasted_iota(jnp.int32, (capacity, lanes), 1)
    for t in range(tensors):
        own = jnp.where(pick, jnp.broadcast_to(inv[t:t + 1], pick.shape), 0.0)
        inverse[t] = jnp.broadcast_to(jnp.sum(own, axis=1, keepdims=True), pick.shape)
    small = [
        pltpu.make_async_copy(scale_ref, scale_out, small_sem.at[0]),
        pltpu.make_async_copy(energy_ref, energy_out, small_sem.at[1]),
    ]
    for copy in small:
        copy.start()

    for t in range(tensors):
        def scaled(j, carry, t=t, swap=False):
            factor = jnp.broadcast_to(inverse[t, pl.ds(j, 1), :], (8, lanes))
            for p in range(SIDE):
                for q in range(SIDE):
                    r = (q * SIDE + p) if swap else (p * SIDE + q)
                    for w in range(0, outb.shape[3], lanes):
                        at = slice(w, w + lanes)
                        part = y2_ref[p, t, j - a, q, :, at] if swap else x2_ref[p, t, j, q, :, at]
                        outb[t, j, r * 8:r * 8 + 8, at] = part * factor
            put(t, j, outb.at[t, j]).start()
            return carry

        lax.fori_loop(0, a, functools.partial(scaled, swap=False), 0)
        lax.fori_loop(a, n, functools.partial(scaled, swap=True), 0)
    for t in range(tensors):
        lax.fori_loop(0, capacity, lambda j, _: (put(t, j, zeros).wait(), _)[1], 0)
    for copy in small:
        copy.wait()


def on_device(moments, owner_counts):
    tensors, blocks, sub, width = moments.shape
    groups, cols = lax.axis_size("row"), lax.axis_size("col")
    capacity = 2 * HALF
    f32, i32 = jnp.float32, jnp.int32
    smem = pl.BlockSpec(memory_space=pltpu.SMEM)
    hbm = pl.BlockSpec(memory_space=pl.ANY)
    vmem = pl.BlockSpec(memory_space=pltpu.VMEM)

    plan, tier = pl.pallas_call(
        plan_kernel,
        out_shape=(jax.ShapeDtypeStruct((128,), i32), jax.ShapeDtypeStruct((1,), i32)),
        in_specs=[smem],
        out_specs=(smem, smem),
        name="plan",
    )(owner_counts)

    def branch(number, slots):
        arrived = pltpu.VMEM((SIDE, tensors, HALF, SIDE, sub, width), f32)
        got = pltpu.VMEM((SIDE, slots, sub, width), f32)
        sent = pltpu.VMEM((tensors, SIDE - 1, slots, sub, width), f32)
        out = pltpu.VMEM((tensors, SIDE - 1, HALF, SIDE, sub, width), f32)
        stat = pltpu.VMEM((8, blocks), f32)
        dma = pltpu.SemaphoreType.DMA
        peers = max(cols - 1, 1)
        piece = 4 * sub * width
        limit = piece * (2 * blocks + 28 * slots + 48 * HALF) + 1 * 2**20

        def run(moments, plan):
            x2, y2, stats = pl.pallas_call(
                functools.partial(move_kernel, slots, cols),
                out_shape=(arrived, arrived, jax.ShapeDtypeStruct((8, blocks), f32)),
                in_specs=[hbm, hbm],
                out_specs=(vmem, vmem, vmem),
                scratch_shapes=[
                    pltpu.VMEM((blocks, sub, width), f32), pltpu.VMEM((blocks, sub, width), f32),
                    sent, sent, got, got, got, got, out, out,
                    pltpu.VMEM((4, blocks, 128), f32), stat, stat, stat,
                    pltpu.VMEM((peers, 8, blocks), f32),
                    pltpu.VMEM((SIDE - 1, 8, blocks), f32),
                    pltpu.VMEM((SIDE - 1, 8, blocks), f32),
                    pltpu.SMEM((128,), i32), dma, dma((2,)), dma((2, 2, 3)), dma((2, 2, 3)), dma((2, 2, 3)), dma((2, 2, 3)),
                    dma((peers,)), dma((peers,)), dma((2, 3)), dma((2, 3)),
                ],
                compiler_params=pltpu.CompilerParams(
                    collective_id=number, has_side_effects=True, vmem_limit_bytes=limit),
                name=f"move{slots}",
            )(plan, moments)
            return pl.pallas_call(
                functools.partial(place_kernel, float(sub * groups * width * cols)),
                out_shape=(
                    jax.ShapeDtypeStruct((tensors, capacity * sub * groups, width), f32),
                    jax.ShapeDtypeStruct((tensors, capacity), f32),
                    jax.ShapeDtypeStruct((tensors, capacity), f32),
                ),
                in_specs=[smem, vmem, vmem, vmem],
                out_specs=(hbm, hbm, hbm),
                scratch_shapes=[
                    pltpu.VMEM((tensors, capacity, sub * groups, width), f32),
                    pltpu.VMEM((sub * groups, width), f32),
                    pltpu.VMEM((tensors, capacity, 128), f32),
                    pltpu.VMEM((tensors, capacity), f32), pltpu.VMEM((tensors, capacity), f32),
                    dma((tensors, capacity)), dma((2,)),
                ],
                compiler_params=pltpu.CompilerParams(vmem_limit_bytes=16 * 2**20),
                name="place",
            )(plan, stats, x2, y2)

        return run

    return lax.switch(tier[0], [branch(i, s) for i, s in enumerate(TIERS)], moments, plan)


def solution(mesh):
    placed = (P(None, None, "row", "col"), P())
    return jax.shard_map(
        on_device,
        mesh=mesh,
        in_specs=placed,
        out_specs=(P(None, "row", "col"), P(None, "row"), P(None, "row")),
        check_vma=False,
    )
```

```python
import functools
import jax
import jax.numpy as jnp
from jax import lax
from jax.sharding import PartitionSpec as P
from jax.experimental import pallas as pl
from jax.experimental.pallas import tpu as pltpu

SIDE = 4
GROUPS = SIDE * SIDE
HALF = 8
TIERS = (17, 18, 19, 20, 21, 22, 23, 24, 26, 28, 32)
MESH = pl.DeviceIdType.MESH
TURNS = (1, 3, 2)


def plan_kernel(count_ref, plan_ref, tier_ref):
    groups = SIDE * SIDE
    n = [count_ref[g] for g in range(groups)]
    low = [jnp.maximum(v - HALF, 0) for v in n]
    high = [jnp.minimum(v, HALF) for v in n]
    a = [(n[g] + (g // SIDE + g % SIDE) % 2) // 2 for g in range(groups)]
    col = [sum(a[x::SIDE]) for x in range(SIDE)]
    row = [sum(n[y * SIDE:(y + 1) * SIDE]) - sum(a[y * SIDE:(y + 1) * SIDE]) for y in range(SIDE)]
    for _ in range(2):
        for g in range(groups):
            y, x = divmod(g, SIDE)
            new = jnp.clip(a[g] - ((col[x] - row[y] + 1) >> 1), low[g], high[g])
            col[x] = col[x] + new - a[g]
            row[y] = row[y] + a[g] - new
            a[g] = new
    need = functools.reduce(jnp.maximum, col + row)
    tier = jnp.int32(0)
    for limit in TIERS[:-1]:
        tier = tier + (need > limit).astype(jnp.int32)
    tier_ref[0] = tier
    start = jnp.int32(0)
    at_x, at_y = [jnp.int32(0)] * SIDE, [jnp.int32(0)] * SIDE
    for g in range(groups):
        y, x = divmod(g, SIDE)
        plan_ref[g] = a[g]
        plan_ref[groups + g] = start
        plan_ref[2 * groups + g] = at_x[x]
        plan_ref[3 * groups + g] = at_y[y]
        plan_ref[4 * groups + g] = n[g]
        start = start + n[g]
        at_x[x] = at_x[x] + a[g]
        at_y[y] = at_y[y] + n[g] - a[g]


def move_kernel(
    slots, cols, plan_in, moments_ref, x2_ref, y2_ref, stats_ref,
    mom0, mom1, send_x, send_y, got_x0, got_x1, got_y0, got_y1, out_x, out_y,
    pieces, stat_a, stat_b, stat_c, all_a, all_b, all_c,
    plan_ref, go_sem, plan_sem, load_sem, send1, recv1, send2, recv2, sa, ra, sb, rb,
):
    mom = (mom0, mom1)
    got_x = (got_x0, got_x1)
    got_y = (got_y0, got_y1)
    tensors = 2
    me = lax.axis_index("row")
    c = lax.axis_index("col")
    y, x = me // SIDE, me % SIDE
    blocks = mom0.shape[0]

    loads = [
        pltpu.make_async_copy(moments_ref.at[t], mom[t], load_sem.at[t])
        for t in range(tensors)
    ]
    table = pltpu.make_async_copy(plan_in, plan_ref, plan_sem)
    table.start()
    for load in loads:
        load.start()

    def x_peer(d):
        return {"row": y * SIDE + (x + d) % SIDE}

    def y_peer(d):
        return {"row": ((y + d) % SIDE) * SIDE + x}

    core, z, planes = c % 2, c // 2, cols // 2
    mate = {"col": z * 2 + 1 - core}
    barrier = pltpu.get_barrier_semaphore()
    for d in TURNS:
        pl.semaphore_signal(barrier, inc=1, device_id={**x_peer(d), "col": z * 2}, device_id_type=MESH)
        pl.semaphore_signal(barrier, inc=1, device_id={**y_peer(d), "col": z * 2}, device_id_type=MESH)
    for d in range(1, planes):
        pl.semaphore_signal(
            barrier, inc=1, device_id={"col": ((z + d) % planes) * 2 + 1}, device_id_type=MESH)
    pl.semaphore_signal(barrier, inc=1, device_id=mate, device_id_type=MESH)

    def order_x(xd):
        at = [plan_ref[2 * GROUPS + i * SIDE + xd] for i in range(SIDE)]
        base = [plan_ref[GROUPS + i * SIDE + xd] - at[i] for i in range(SIDE)]

        def block_of(k):
            b = base[0]
            for i in range(1, SIDE):
                b = jnp.where(k >= at[i], base[i], b)
            return jnp.clip(b + k, 0, blocks - 1)

        return block_of

    def order_y(yd):
        at = [plan_ref[3 * GROUPS + yd * SIDE + i] for i in range(SIDE)]
        base = [
            plan_ref[GROUPS + yd * SIDE + i] + plan_ref[yd * SIDE + i] - at[i]
            for i in range(SIDE)
        ]

        def block_of(k):
            b = base[0]
            for i in range(1, SIDE):
                b = jnp.where(k >= at[i], base[i], b)
            return jnp.clip(b + k, 0, blocks - 1)

        return block_of

    def pack1(t, block_of, dst):
        def step(k, carry):
            dst[k] = mom[t][block_of(k)]
            return carry

        lax.fori_loop(0, slots, step, 0, unroll=2)

    table.wait()

    @pl.when(core == 0)
    def _():
        pl.semaphore_wait(barrier, 4 * (SIDE - 1) + 1)
        pl.semaphore_signal(go_sem, inc=1, device_id=mate, device_id_type=MESH)

    @pl.when(core == 1)
    def _():
        pl.semaphore_wait(go_sem, 1)

    first = [[], []]
    for t in range(tensors):
        loads[t].wait()
        for i, d in enumerate(TURNS):
            pack1(t, order_x((x + d) % SIDE), send_x.at[t, i])
            copy = pltpu.make_async_remote_copy(
                send_x.at[t, i], got_x[t].at[x], send1.at[t, 0, i], recv1.at[t, 0, i],
                device_id=x_peer(d), device_id_type=MESH)
            copy.start()
            first[t].append(copy)
            pack1(t, order_y((y + d) % SIDE), send_y.at[t, i])
            copy = pltpu.make_async_remote_copy(
                send_y.at[t, i], got_y[t].at[y], send1.at[t, 1, i], recv1.at[t, 1, i],
                device_id=y_peer(d), device_id_type=MESH)
            copy.start()
            first[t].append(copy)
        pack1(t, order_x(x), got_x[t].at[x])
        pack1(t, order_y(y), got_y[t].at[y])

    width = mom0.shape[2]
    for t in range(tensors):
        def measure(k, carry, t=t):
            rows = pl.ds(pl.multiple_of(k * 8, 8), 8)
            peak = None
            for w in range(0, width, 128):
                v = mom[t][rows, :, w:w + 128]
                m, q = jnp.abs(v), v * v
                peak, total = (m, q) if peak is None else (jnp.maximum(peak, m), total + q)
            pieces[t, rows, :] = jnp.max(peak, axis=1)
            pieces[2 + t, rows, :] = jnp.sum(total, axis=1)
            return carry

        lax.fori_loop(0, blocks // 8, measure, 0)
    stat_a[...] = jnp.zeros_like(stat_a)
    for t in range(tensors):
        stat_a[t:t + 1, :] = jnp.max(pieces[t].T, axis=0, keepdims=True)
        stat_a[2 + t:3 + t, :] = jnp.sum(pieces[2 + t].T, axis=0, keepdims=True)
    is_peak = lax.broadcasted_iota(jnp.int32, stat_a.shape, 0) < tensors

    def join(mine, others, n):
        v = mine[...]
        for i in range(n):
            o = others[i]
            v = jnp.where(is_peak, jnp.maximum(v, o), v + o)
        return v


    @pl.when(core == 1)
    def _():
        pl.semaphore_wait(barrier, 2 * planes - 1)
        pl.semaphore_signal(go_sem, inc=1, device_id=mate, device_id_type=MESH)

    @pl.when(core == 0)
    def _():
        pl.semaphore_wait(go_sem, 1)

    stage = []
    for d in range(1, cols):
        copy = pltpu.make_async_remote_copy(
            stat_a, all_a.at[d - 1], sa.at[d - 1], ra.at[d - 1],
            device_id={"col": (c + d) % cols}, device_id_type=MESH)
        copy.start()
        stage.append(copy)
    for copy in stage:
        copy.wait()
    stat_b[...] = join(stat_a, all_a, cols - 1)
    stage = []
    for i, d in enumerate(TURNS):
        copy = pltpu.make_async_remote_copy(
            stat_b, all_b.at[i], sb.at[0, i], rb.at[0, i],
            device_id=x_peer(d), device_id_type=MESH)
        copy.start()
        stage.append(copy)

    def pack2(got, offset, dst):
        def step(j, carry):
            k = jnp.minimum(offset + j, slots - 1)
            for s in range(SIDE):
                dst[j, s] = got[s, k]
            return carry

        lax.fori_loop(0, HALF, step, 0)

    second = []
    for t in range(tensors):
        for copy in first[t]:
            copy.wait_recv()
        if t == 1:
            for copy in stage:
                copy.wait()
            stat_c[...] = join(stat_b, all_b, SIDE - 1)
            stage = []
            for i, d in enumerate(TURNS):
                copy = pltpu.make_async_remote_copy(
                    stat_c, all_c.at[i], sb.at[1, i], rb.at[1, i],
                    device_id=y_peer(d), device_id_type=MESH)
                copy.start()
                stage.append(copy)
        for i, d in enumerate(TURNS):
            yd, xd = (y + d) % SIDE, (x + d) % SIDE
            pack2(got_x[t], plan_ref[2 * GROUPS + yd * SIDE + x], out_x.at[t, i])
            copy = pltpu.make_async_remote_copy(
                out_x.at[t, i], x2_ref.at[y, t], send2.at[t, 0, i], recv2.at[t, 0, i],
                device_id=y_peer(d), device_id_type=MESH)
            copy.start()
            second.append(copy)
            pack2(got_y[t], plan_ref[3 * GROUPS + y * SIDE + xd], out_y.at[t, i])
            copy = pltpu.make_async_remote_copy(
                out_y.at[t, i], y2_ref.at[x, t], send2.at[t, 1, i], recv2.at[t, 1, i],
                device_id=x_peer(d), device_id_type=MESH)
            copy.start()
            second.append(copy)
        pack2(got_x[t], plan_ref[2 * GROUPS + me], x2_ref.at[y, t])
        pack2(got_y[t], plan_ref[3 * GROUPS + me], y2_ref.at[x, t])

    for t in range(tensors):
        for copy in first[t]:
            copy.wait_send()
    for copy in stage:
        copy.wait()
    stats_ref[...] = join(stat_c, all_c, SIDE - 1)
    for copy in second:
        copy.wait()


def place_kernel(
    full_size, plan_ref, stats_ref, x2_ref, y2_ref, norm_ref, scale_out, energy_out,
    outb, zeros, inverse, scale_ref, energy_ref, out_sem, small_sem,
):
    tensors, capacity = scale_ref.shape
    me = lax.axis_index("row")
    a, start, n = plan_ref[me], plan_ref[GROUPS + me], plan_ref[4 * GROUPS + me]
    zeros[...] = jnp.zeros_like(zeros)
    rows = zeros.shape[0]

    def put(t, j, src):
        at = pl.ds(pl.multiple_of(j * rows, rows), rows)
        return pltpu.make_async_copy(src, norm_ref.at[t, at], out_sem.at[t, j])

    for t in range(tensors):
        lax.fori_loop(n, capacity, lambda j, _: (put(t, j, zeros).start(), _)[1], 0)

    lanes = stats_ref.shape[1]
    mine = pltpu.roll(stats_ref[...], lax.rem(lanes - start, lanes), 1)
    lane = lax.broadcasted_iota(jnp.int32, mine.shape, 1)
    scale = jnp.where(lane < n, jnp.maximum(mine, 1.0), 1.0)
    energy = jnp.where(lane < n, mine / full_size, 0.0)
    scale_ref[...] = scale[:tensors, :capacity]
    energy_ref[...] = energy[tensors:2 * tensors, :capacity]
    inv = 1.0 / scale
    pick = lax.broadcasted_iota(jnp.int32, (capacity, lanes), 0)
    pick = pick == lax.broadcasted_iota(jnp.int32, (capacity, lanes), 1)
    for t in range(tensors):
        own = jnp.where(pick, jnp.broadcast_to(inv[t:t + 1], pick.shape), 0.0)
        inverse[t] = jnp.broadcast_to(jnp.sum(own, axis=1, keepdims=True), pick.shape)
    small = [
        pltpu.make_async_copy(scale_ref, scale_out, small_sem.at[0]),
        pltpu.make_async_copy(energy_ref, energy_out, small_sem.at[1]),
    ]
    for copy in small:
        copy.start()

    for t in range(tensors):
        def scaled(j, carry, t=t, swap=False):
            factor = jnp.broadcast_to(inverse[t, pl.ds(j, 1), :], (8, lanes))
            for p in range(SIDE):
                for q in range(SIDE):
                    r = (q * SIDE + p) if swap else (p * SIDE + q)
                    for w in range(0, outb.shape[3], lanes):
                        at = slice(w, w + lanes)
                        part = y2_ref[p, t, j - a, q, :, at] if swap else x2_ref[p, t, j, q, :, at]
                        outb[t, j, r * 8:r * 8 + 8, at] = part * factor
            put(t, j, outb.at[t, j]).start()
            return carry

        lax.fori_loop(0, a, functools.partial(scaled, swap=False), 0)
        lax.fori_loop(a, n, functools.partial(scaled, swap=True), 0)
    for t in range(tensors):
        lax.fori_loop(0, capacity, lambda j, _: (put(t, j, zeros).wait(), _)[1], 0)
    for copy in small:
        copy.wait()


def on_device(moments, owner_counts):
    tensors, blocks, sub, width = moments.shape
    groups, cols = lax.axis_size("row"), lax.axis_size("col")
    capacity = 2 * HALF
    f32, i32 = jnp.float32, jnp.int32
    smem = pl.BlockSpec(memory_space=pltpu.SMEM)
    hbm = pl.BlockSpec(memory_space=pl.ANY)
    vmem = pl.BlockSpec(memory_space=pltpu.VMEM)

    plan, tier = pl.pallas_call(
        plan_kernel,
        out_shape=(jax.ShapeDtypeStruct((128,), i32), jax.ShapeDtypeStruct((1,), i32)),
        in_specs=[smem],
        out_specs=(smem, smem),
        name="plan",
    )(owner_counts)

    def branch(number, slots):
        arrived = pltpu.VMEM((SIDE, tensors, HALF, SIDE, sub, width), f32)
        got = pltpu.VMEM((SIDE, slots, sub, width), f32)
        sent = pltpu.VMEM((tensors, SIDE - 1, slots, sub, width), f32)
        out = pltpu.VMEM((tensors, SIDE - 1, HALF, SIDE, sub, width), f32)
        stat = pltpu.VMEM((8, blocks), f32)
        dma = pltpu.SemaphoreType.DMA
        peers = max(cols - 1, 1)
        piece = 4 * sub * width
        limit = piece * (2 * blocks + 28 * slots + 48 * HALF) + 1 * 2**20

        def run(moments, plan):
            x2, y2, stats = pl.pallas_call(
                functools.partial(move_kernel, slots, cols),
                out_shape=(arrived, arrived, jax.ShapeDtypeStruct((8, blocks), f32)),
                in_specs=[hbm, hbm],
                out_specs=(vmem, vmem, vmem),
                scratch_shapes=[
                    pltpu.VMEM((blocks, sub, width), f32), pltpu.VMEM((blocks, sub, width), f32),
                    sent, sent, got, got, got, got, out, out,
                    pltpu.VMEM((4, blocks, 128), f32), stat, stat, stat,
                    pltpu.VMEM((peers, 8, blocks), f32),
                    pltpu.VMEM((SIDE - 1, 8, blocks), f32),
                    pltpu.VMEM((SIDE - 1, 8, blocks), f32),
                    pltpu.SMEM((128,), i32), pltpu.SemaphoreType.REGULAR, dma, dma((2,)), dma((2, 2, 3)), dma((2, 2, 3)), dma((2, 2, 3)), dma((2, 2, 3)),
                    dma((peers,)), dma((peers,)), dma((2, 3)), dma((2, 3)),
                ],
                compiler_params=pltpu.CompilerParams(
                    collective_id=number, has_side_effects=True, vmem_limit_bytes=limit),
                name=f"move{slots}",
            )(plan, moments)
            return pl.pallas_call(
                functools.partial(place_kernel, float(sub * groups * width * cols)),
                out_shape=(
                    jax.ShapeDtypeStruct((tensors, capacity * sub * groups, width), f32),
                    jax.ShapeDtypeStruct((tensors, capacity), f32),
                    jax.ShapeDtypeStruct((tensors, capacity), f32),
                ),
                in_specs=[smem, vmem, vmem, vmem],
                out_specs=(hbm, hbm, hbm),
                scratch_shapes=[
                    pltpu.VMEM((tensors, capacity, sub * groups, width), f32),
                    pltpu.VMEM((sub * groups, width), f32),
                    pltpu.VMEM((tensors, capacity, 128), f32),
                    pltpu.VMEM((tensors, capacity), f32), pltpu.VMEM((tensors, capacity), f32),
                    dma((tensors, capacity)), dma((2,)),
                ],
                compiler_params=pltpu.CompilerParams(vmem_limit_bytes=16 * 2**20),
                name="place",
            )(plan, stats, x2, y2)

        return run

    return lax.switch(tier[0], [branch(i, s) for i, s in enumerate(TIERS)], moments, plan)


def solution(mesh):
    placed = (P(None, None, "row", "col"), P())
    return jax.shard_map(
        on_device,
        mesh=mesh,
        in_specs=placed,
        out_specs=(P(None, "row", "col"), P(None, "row"), P(None, "row")),
        check_vma=False,
    )
```

```python
import functools
import jax
import jax.numpy as jnp
from jax import lax
from jax.sharding import PartitionSpec as P
from jax.experimental import pallas as pl
from jax.experimental.pallas import tpu as pltpu

SIDE = 4
GROUPS = SIDE * SIDE
HALF = 8
TIERS = (17, 18, 19, 20, 21, 22, 23, 24, 26, 28, 32)
MESH = pl.DeviceIdType.MESH
TURNS = (1, 3, 2)


def plan_kernel(count_ref, plan_ref, tier_ref):
    groups = SIDE * SIDE
    n = [count_ref[g] for g in range(groups)]
    low = [jnp.maximum(v - HALF, 0) for v in n]
    high = [jnp.minimum(v, HALF) for v in n]
    a = [(n[g] + (g // SIDE + g % SIDE) % 2) // 2 for g in range(groups)]
    col = [sum(a[x::SIDE]) for x in range(SIDE)]
    row = [sum(n[y * SIDE:(y + 1) * SIDE]) - sum(a[y * SIDE:(y + 1) * SIDE]) for y in range(SIDE)]
    for _ in range(2):
        for g in range(groups):
            y, x = divmod(g, SIDE)
            new = jnp.clip(a[g] - ((col[x] - row[y] + 1) >> 1), low[g], high[g])
            col[x] = col[x] + new - a[g]
            row[y] = row[y] + a[g] - new
            a[g] = new
    need = functools.reduce(jnp.maximum, col + row)
    tier = jnp.int32(0)
    for limit in TIERS[:-1]:
        tier = tier + (need > limit).astype(jnp.int32)
    tier_ref[0] = tier
    start = jnp.int32(0)
    at_x, at_y = [jnp.int32(0)] * SIDE, [jnp.int32(0)] * SIDE
    for g in range(groups):
        y, x = divmod(g, SIDE)
        plan_ref[g] = a[g]
        plan_ref[groups + g] = start
        plan_ref[2 * groups + g] = at_x[x]
        plan_ref[3 * groups + g] = at_y[y]
        plan_ref[4 * groups + g] = n[g]
        start = start + n[g]
        at_x[x] = at_x[x] + a[g]
        at_y[y] = at_y[y] + n[g] - a[g]


def move_kernel(
    slots, cols, plan_ref, moments_ref, x2_ref, y2_ref, stats_ref,
    mom0, mom1, send_x, send_y, got_x0, got_x1, got_y0, got_y1, out_x, out_y,
    pieces, stat_a, stat_b, stat_c, all_a, all_b, all_c,
    go_sem, load_sem, send1, recv1, send2, recv2, sa, ra, sb, rb,
):
    mom = (mom0, mom1)
    got_x = (got_x0, got_x1)
    got_y = (got_y0, got_y1)
    tensors = 2
    me = lax.axis_index("row")
    c = lax.axis_index("col")
    y, x = me // SIDE, me % SIDE
    blocks = mom0.shape[0]

    loads = [
        pltpu.make_async_copy(moments_ref.at[t], mom[t], load_sem.at[t])
        for t in range(tensors)
    ]
    for load in loads:
        load.start()

    def x_peer(d):
        return {"row": y * SIDE + (x + d) % SIDE}

    def y_peer(d):
        return {"row": ((y + d) % SIDE) * SIDE + x}

    core, z, planes = c % 2, c // 2, cols // 2
    mate = {"col": z * 2 + 1 - core}
    barrier = pltpu.get_barrier_semaphore()
    for d in TURNS:
        pl.semaphore_signal(barrier, inc=1, device_id={**x_peer(d), "col": z * 2}, device_id_type=MESH)
        pl.semaphore_signal(barrier, inc=1, device_id={**y_peer(d), "col": z * 2}, device_id_type=MESH)
    for d in range(1, planes):
        pl.semaphore_signal(
            barrier, inc=1, device_id={"col": ((z + d) % planes) * 2 + 1}, device_id_type=MESH)
    pl.semaphore_signal(barrier, inc=1, device_id=mate, device_id_type=MESH)

    def order_x(xd):
        at = [plan_ref[2 * GROUPS + i * SIDE + xd] for i in range(SIDE)]
        base = [plan_ref[GROUPS + i * SIDE + xd] - at[i] for i in range(SIDE)]

        def block_of(k):
            b = base[0]
            for i in range(1, SIDE):
                b = jnp.where(k >= at[i], base[i], b)
            return jnp.clip(b + k, 0, blocks - 1)

        return block_of

    def order_y(yd):
        at = [plan_ref[3 * GROUPS + yd * SIDE + i] for i in range(SIDE)]
        base = [
            plan_ref[GROUPS + yd * SIDE + i] + plan_ref[yd * SIDE + i] - at[i]
            for i in range(SIDE)
        ]

        def block_of(k):
            b = base[0]
            for i in range(1, SIDE):
                b = jnp.where(k >= at[i], base[i], b)
            return jnp.clip(b + k, 0, blocks - 1)

        return block_of

    def pack1(t, block_of, dst):
        def step(k, carry):
            dst[k] = mom[t][block_of(k)]
            return carry

        lax.fori_loop(0, slots, step, 0, unroll=2)


    @pl.when(core == 0)
    def _():
        pl.semaphore_wait(barrier, 4 * (SIDE - 1) + 1)
        pl.semaphore_signal(go_sem, inc=1, device_id=mate, device_id_type=MESH)

    @pl.when(core == 1)
    def _():
        pl.semaphore_wait(go_sem, 1)

    first = [[], []]
    for t in range(tensors):
        loads[t].wait()
        for i, d in enumerate(TURNS):
            pack1(t, order_x((x + d) % SIDE), send_x.at[t, i])
            copy = pltpu.make_async_remote_copy(
                send_x.at[t, i], got_x[t].at[x], send1.at[t, 0, i], recv1.at[t, 0, i],
                device_id=x_peer(d), device_id_type=MESH)
            copy.start()
            first[t].append(copy)
            pack1(t, order_y((y + d) % SIDE), send_y.at[t, i])
            copy = pltpu.make_async_remote_copy(
                send_y.at[t, i], got_y[t].at[y], send1.at[t, 1, i], recv1.at[t, 1, i],
                device_id=y_peer(d), device_id_type=MESH)
            copy.start()
            first[t].append(copy)
        pack1(t, order_x(x), got_x[t].at[x])
        pack1(t, order_y(y), got_y[t].at[y])

    width = mom0.shape[2]
    for t in range(tensors):
        def measure(k, carry, t=t):
            rows = pl.ds(pl.multiple_of(k * 8, 8), 8)
            peak = None
            for w in range(0, width, 128):
                v = mom[t][rows, :, w:w + 128]
                m, q = jnp.abs(v), v * v
                peak, total = (m, q) if peak is None else (jnp.maximum(peak, m), total + q)
            pieces[t, rows, :] = jnp.max(peak, axis=1)
            pieces[2 + t, rows, :] = jnp.sum(total, axis=1)
            return carry

        lax.fori_loop(0, blocks // 8, measure, 0)
    stat_a[...] = jnp.zeros_like(stat_a)
    for t in range(tensors):
        stat_a[t:t + 1, :] = jnp.max(pieces[t].T, axis=0, keepdims=True)
        stat_a[2 + t:3 + t, :] = jnp.sum(pieces[2 + t].T, axis=0, keepdims=True)
    is_peak = lax.broadcasted_iota(jnp.int32, stat_a.shape, 0) < tensors

    def join(mine, others, n):
        v = mine[...]
        for i in range(n):
            o = others[i]
            v = jnp.where(is_peak, jnp.maximum(v, o), v + o)
        return v


    @pl.when(core == 1)
    def _():
        pl.semaphore_wait(barrier, 2 * planes - 1)
        pl.semaphore_signal(go_sem, inc=1, device_id=mate, device_id_type=MESH)

    @pl.when(core == 0)
    def _():
        pl.semaphore_wait(go_sem, 1)

    stage = []
    for d in range(1, cols):
        copy = pltpu.make_async_remote_copy(
            stat_a, all_a.at[d - 1], sa.at[d - 1], ra.at[d - 1],
            device_id={"col": (c + d) % cols}, device_id_type=MESH)
        copy.start()
        stage.append(copy)
    for copy in stage:
        copy.wait()
    stat_b[...] = join(stat_a, all_a, cols - 1)
    stage = []
    for i, d in enumerate(TURNS):
        copy = pltpu.make_async_remote_copy(
            stat_b, all_b.at[i], sb.at[0, i], rb.at[0, i],
            device_id=x_peer(d), device_id_type=MESH)
        copy.start()
        stage.append(copy)

    def pack2(got, offset, dst):
        def step(j, carry):
            k = jnp.minimum(offset + j, slots - 1)
            for s in range(SIDE):
                dst[j, s] = got[s, k]
            return carry

        lax.fori_loop(0, HALF, step, 0)

    second = []
    for t in range(tensors):
        for copy in first[t]:
            copy.wait_recv()
        if t == 1:
            for copy in stage:
                copy.wait()
            stat_c[...] = join(stat_b, all_b, SIDE - 1)
            stage = []
            for i, d in enumerate(TURNS):
                copy = pltpu.make_async_remote_copy(
                    stat_c, all_c.at[i], sb.at[1, i], rb.at[1, i],
                    device_id=y_peer(d), device_id_type=MESH)
                copy.start()
                stage.append(copy)
        for i, d in enumerate(TURNS):
            yd, xd = (y + d) % SIDE, (x + d) % SIDE
            pack2(got_x[t], plan_ref[2 * GROUPS + yd * SIDE + x], out_x.at[t, i])
            copy = pltpu.make_async_remote_copy(
                out_x.at[t, i], x2_ref.at[y, t], send2.at[t, 0, i], recv2.at[t, 0, i],
                device_id=y_peer(d), device_id_type=MESH)
            copy.start()
            second.append(copy)
            pack2(got_y[t], plan_ref[3 * GROUPS + y * SIDE + xd], out_y.at[t, i])
            copy = pltpu.make_async_remote_copy(
                out_y.at[t, i], y2_ref.at[x, t], send2.at[t, 1, i], recv2.at[t, 1, i],
                device_id=x_peer(d), device_id_type=MESH)
            copy.start()
            second.append(copy)
        pack2(got_x[t], plan_ref[2 * GROUPS + me], x2_ref.at[y, t])
        pack2(got_y[t], plan_ref[3 * GROUPS + me], y2_ref.at[x, t])

    for t in range(tensors):
        for copy in first[t]:
            copy.wait_send()
    for copy in stage:
        copy.wait()
    stats_ref[...] = join(stat_c, all_c, SIDE - 1)
    for copy in second:
        copy.wait()


def place_kernel(
    full_size, plan_ref, stats_ref, x2_ref, y2_ref, norm_ref, scale_out, energy_out,
    outb, zeros, inverse, scale_ref, energy_ref, out_sem, small_sem,
):
    tensors, capacity = scale_ref.shape
    me = lax.axis_index("row")
    a, start, n = plan_ref[me], plan_ref[GROUPS + me], plan_ref[4 * GROUPS + me]
    zeros[...] = jnp.zeros_like(zeros)
    rows = zeros.shape[0]

    def put(t, j, src):
        at = pl.ds(pl.multiple_of(j * rows, rows), rows)
        return pltpu.make_async_copy(src, norm_ref.at[t, at], out_sem.at[t, j])

    for t in range(tensors):
        lax.fori_loop(n, capacity, lambda j, _: (put(t, j, zeros).start(), _)[1], 0)

    lanes = stats_ref.shape[1]
    mine = pltpu.roll(stats_ref[...], lax.rem(lanes - start, lanes), 1)
    lane = lax.broadcasted_iota(jnp.int32, mine.shape, 1)
    scale = jnp.where(lane < n, jnp.maximum(mine, 1.0), 1.0)
    energy = jnp.where(lane < n, mine / full_size, 0.0)
    scale_ref[...] = scale[:tensors, :capacity]
    energy_ref[...] = energy[tensors:2 * tensors, :capacity]
    inv = 1.0 / scale
    pick = lax.broadcasted_iota(jnp.int32, (capacity, lanes), 0)
    pick = pick == lax.broadcasted_iota(jnp.int32, (capacity, lanes), 1)
    for t in range(tensors):
        own = jnp.where(pick, jnp.broadcast_to(inv[t:t + 1], pick.shape), 0.0)
        inverse[t] = jnp.broadcast_to(jnp.sum(own, axis=1, keepdims=True), pick.shape)
    small = [
        pltpu.make_async_copy(scale_ref, scale_out, small_sem.at[0]),
        pltpu.make_async_copy(energy_ref, energy_out, small_sem.at[1]),
    ]
    for copy in small:
        copy.start()

    for t in range(tensors):
        def scaled(j, carry, t=t, swap=False):
            factor = jnp.broadcast_to(inverse[t, pl.ds(j, 1), :], (8, lanes))
            for p in range(SIDE):
                for q in range(SIDE):
                    r = (q * SIDE + p) if swap else (p * SIDE + q)
                    for w in range(0, outb.shape[3], lanes):
                        at = slice(w, w + lanes)
                        part = y2_ref[p, t, j - a, q, :, at] if swap else x2_ref[p, t, j, q, :, at]
                        outb[t, j, r * 8:r * 8 + 8, at] = part * factor
            put(t, j, outb.at[t, j]).start()
            return carry

        lax.fori_loop(0, a, functools.partial(scaled, swap=False), 0)
        lax.fori_loop(a, n, functools.partial(scaled, swap=True), 0)
    for t in range(tensors):
        lax.fori_loop(0, capacity, lambda j, _: (put(t, j, zeros).wait(), _)[1], 0)
    for copy in small:
        copy.wait()


def on_device(moments, owner_counts):
    tensors, blocks, sub, width = moments.shape
    groups, cols = lax.axis_size("row"), lax.axis_size("col")
    capacity = 2 * HALF
    f32, i32 = jnp.float32, jnp.int32
    smem = pl.BlockSpec(memory_space=pltpu.SMEM)
    hbm = pl.BlockSpec(memory_space=pl.ANY)
    vmem = pl.BlockSpec(memory_space=pltpu.VMEM)

    plan, tier = pl.pallas_call(
        plan_kernel,
        out_shape=(pltpu.SMEM((128,), i32), pltpu.SMEM((1,), i32)),
        in_specs=[smem],
        out_specs=(smem, smem),
        name="plan",
    )(owner_counts)

    def branch(number, slots):
        arrived = pltpu.VMEM((SIDE, tensors, HALF, SIDE, sub, width), f32)
        got = pltpu.VMEM((SIDE, slots, sub, width), f32)
        sent = pltpu.VMEM((tensors, SIDE - 1, slots, sub, width), f32)
        out = pltpu.VMEM((tensors, SIDE - 1, HALF, SIDE, sub, width), f32)
        stat = pltpu.VMEM((8, blocks), f32)
        dma = pltpu.SemaphoreType.DMA
        peers = max(cols - 1, 1)
        piece = 4 * sub * width
        limit = piece * (2 * blocks + 28 * slots + 48 * HALF) + 1 * 2**20

        def run(moments, plan):
            x2, y2, stats = pl.pallas_call(
                functools.partial(move_kernel, slots, cols),
                out_shape=(arrived, arrived, jax.ShapeDtypeStruct((8, blocks), f32)),
                in_specs=[smem, hbm],
                out_specs=(vmem, vmem, vmem),
                scratch_shapes=[
                    pltpu.VMEM((blocks, sub, width), f32), pltpu.VMEM((blocks, sub, width), f32),
                    sent, sent, got, got, got, got, out, out,
                    pltpu.VMEM((4, blocks, 128), f32), stat, stat, stat,
                    pltpu.VMEM((peers, 8, blocks), f32),
                    pltpu.VMEM((SIDE - 1, 8, blocks), f32),
                    pltpu.VMEM((SIDE - 1, 8, blocks), f32),
                    pltpu.SemaphoreType.REGULAR, dma((2,)), dma((2, 2, 3)), dma((2, 2, 3)), dma((2, 2, 3)), dma((2, 2, 3)),
                    dma((peers,)), dma((peers,)), dma((2, 3)), dma((2, 3)),
                ],
                compiler_params=pltpu.CompilerParams(
                    collective_id=number, has_side_effects=True, vmem_limit_bytes=limit),
                name=f"move{slots}",
            )(plan, moments)
            return pl.pallas_call(
                functools.partial(place_kernel, float(sub * groups * width * cols)),
                out_shape=(
                    jax.ShapeDtypeStruct((tensors, capacity * sub * groups, width), f32),
                    jax.ShapeDtypeStruct((tensors, capacity), f32),
                    jax.ShapeDtypeStruct((tensors, capacity), f32),
                ),
                in_specs=[smem, vmem, vmem, vmem],
                out_specs=(hbm, hbm, hbm),
                scratch_shapes=[
                    pltpu.VMEM((tensors, capacity, sub * groups, width), f32),
                    pltpu.VMEM((sub * groups, width), f32),
                    pltpu.VMEM((tensors, capacity, 128), f32),
                    pltpu.VMEM((tensors, capacity), f32), pltpu.VMEM((tensors, capacity), f32),
                    dma((tensors, capacity)), dma((2,)),
                ],
                compiler_params=pltpu.CompilerParams(vmem_limit_bytes=16 * 2**20),
                name="place",
            )(plan, stats, x2, y2)

        return run

    return lax.switch(tier[0], [branch(i, s) for i, s in enumerate(TIERS)], moments, plan)


def solution(mesh):
    placed = (P(None, None, "row", "col"), P())
    return jax.shard_map(
        on_device,
        mesh=mesh,
        in_specs=placed,
        out_specs=(P(None, "row", "col"), P(None, "row"), P(None, "row")),
        check_vma=False,
    )
```

```python
import functools
import jax
import jax.numpy as jnp
from jax import lax
from jax.sharding import PartitionSpec as P
from jax.experimental import pallas as pl
from jax.experimental.pallas import tpu as pltpu

SIDE = 4
GROUPS = SIDE * SIDE
HALF = 8
TIERS = (16, 17, 18, 19, 20, 21, 22, 24, 25, 28, 32)
MESH = pl.DeviceIdType.MESH
TURNS = (1, 3, 2)


def plan_kernel(count_ref, plan_ref, tier_ref):
    groups = SIDE * SIDE
    n = [count_ref[g] for g in range(groups)]
    low = [jnp.maximum(v - HALF, 0) for v in n]
    high = [jnp.minimum(v, HALF) for v in n]
    a = [(n[g] + (g // SIDE + g % SIDE) % 2) // 2 for g in range(groups)]
    col = [sum(a[x::SIDE]) for x in range(SIDE)]
    row = [sum(n[y * SIDE:(y + 1) * SIDE]) - sum(a[y * SIDE:(y + 1) * SIDE]) for y in range(SIDE)]
    for _ in range(3):
        for g in range(groups):
            y, x = divmod(g, SIDE)
            new = jnp.clip(a[g] - ((col[x] - row[y] + 1) >> 1), low[g], high[g])
            col[x] = col[x] + new - a[g]
            row[y] = row[y] + a[g] - new
            a[g] = new
    need = functools.reduce(jnp.maximum, col + row)
    tier = jnp.int32(0)
    for limit in TIERS[:-1]:
        tier = tier + (need > limit).astype(jnp.int32)
    tier_ref[0] = tier
    start = jnp.int32(0)
    at_x, at_y = [jnp.int32(0)] * SIDE, [jnp.int32(0)] * SIDE
    for g in range(groups):
        y, x = divmod(g, SIDE)
        plan_ref[g] = a[g]
        plan_ref[groups + g] = start
        plan_ref[2 * groups + g] = at_x[x]
        plan_ref[3 * groups + g] = at_y[y]
        plan_ref[4 * groups + g] = n[g]
        start = start + n[g]
        at_x[x] = at_x[x] + a[g]
        at_y[y] = at_y[y] + n[g] - a[g]


def move_kernel(
    slots, cols, plan_ref, moments_ref, x2_ref, y2_ref, stats_ref,
    mom0, mom1, send_x, send_y, got_x0, got_x1, got_y0, got_y1, out_x, out_y,
    pieces, stat_a, stat_b, stat_c, all_a, all_b, all_c,
    go_sem, load_sem, send1, recv1, send2, recv2, sa, ra, sb, rb,
):
    mom = (mom0, mom1)
    got_x = (got_x0, got_x1)
    got_y = (got_y0, got_y1)
    tensors = 2
    me = lax.axis_index("row")
    c = lax.axis_index("col")
    y, x = me // SIDE, me % SIDE
    blocks = mom0.shape[0]

    loads = [
        pltpu.make_async_copy(moments_ref.at[t], mom[t], load_sem.at[t])
        for t in range(tensors)
    ]
    for load in loads:
        load.start()

    def x_peer(d):
        return {"row": y * SIDE + (x + d) % SIDE}

    def y_peer(d):
        return {"row": ((y + d) % SIDE) * SIDE + x}

    core, z, planes = c % 2, c // 2, cols // 2
    mate = {"col": z * 2 + 1 - core}
    barrier = pltpu.get_barrier_semaphore()
    for d in TURNS:
        side = z * 2 + (1 if d == 2 else 0)
        pl.semaphore_signal(barrier, inc=1, device_id={**x_peer(d), "col": side}, device_id_type=MESH)
        pl.semaphore_signal(barrier, inc=1, device_id={**y_peer(d), "col": side}, device_id_type=MESH)
    for d in range(1, planes):
        pl.semaphore_signal(
            barrier, inc=1, device_id={"col": ((z + d) % planes) * 2 + 1}, device_id_type=MESH)
    pl.semaphore_signal(barrier, inc=1, device_id=mate, device_id_type=MESH)

    def order_x(xd):
        at = [plan_ref[2 * GROUPS + i * SIDE + xd] for i in range(SIDE)]
        base = [plan_ref[GROUPS + i * SIDE + xd] - at[i] for i in range(SIDE)]

        def block_of(k):
            b = base[0]
            for i in range(1, SIDE):
                b = jnp.where(k >= at[i], base[i], b)
            return jnp.clip(b + k, 0, blocks - 1)

        return block_of

    def order_y(yd):
        at = [plan_ref[3 * GROUPS + yd * SIDE + i] for i in range(SIDE)]
        base = [
            plan_ref[GROUPS + yd * SIDE + i] + plan_ref[yd * SIDE + i] - at[i]
            for i in range(SIDE)
        ]

        def block_of(k):
            b = base[0]
            for i in range(1, SIDE):
                b = jnp.where(k >= at[i], base[i], b)
            return jnp.clip(b + k, 0, blocks - 1)

        return block_of

    def pack1(t, block_of, dst):
        def step(k, carry):
            dst[k] = mom[t][block_of(k)]
            return carry

        lax.fori_loop(0, slots, step, 0, unroll=2)


    @pl.when(core == 0)
    def _():
        pl.semaphore_wait(barrier, 9)
        pl.semaphore_signal(go_sem, inc=1, device_id=mate, device_id_type=MESH)

    @pl.when(core == 1)
    def _():
        pl.semaphore_wait(go_sem, 1)

    first = [[], []]

    def send1_to(t, i, d):
        pack1(t, order_x((x + d) % SIDE), send_x.at[t, i])
        copy = pltpu.make_async_remote_copy(
            send_x.at[t, i], got_x[t].at[x], send1.at[t, 0, i], recv1.at[t, 0, i],
            device_id=x_peer(d), device_id_type=MESH)
        copy.start()
        first[t].append(copy)
        pack1(t, order_y((y + d) % SIDE), send_y.at[t, i])
        copy = pltpu.make_async_remote_copy(
            send_y.at[t, i], got_y[t].at[y], send1.at[t, 1, i], recv1.at[t, 1, i],
            device_id=y_peer(d), device_id_type=MESH)
        copy.start()
        first[t].append(copy)

    for t in range(tensors):
        loads[t].wait()
        for i, d in enumerate(TURNS[:2]):
            send1_to(t, i, d)

    @pl.when(core == 1)
    def _():
        pl.semaphore_wait(barrier, 2 * planes + 3)
        pl.semaphore_signal(go_sem, inc=1, device_id=mate, device_id_type=MESH)

    @pl.when(core == 0)
    def _():
        pl.semaphore_wait(go_sem, 1)

    for t in range(tensors):
        send1_to(t, 2, TURNS[2])
    for t in range(tensors):
        pack1(t, order_x(x), got_x[t].at[x])
        pack1(t, order_y(y), got_y[t].at[y])

    width = mom0.shape[2]
    for t in range(tensors):
        def measure(k, carry, t=t):
            rows = pl.ds(pl.multiple_of(k * 8, 8), 8)
            peak = None
            for w in range(0, width, 128):
                v = mom[t][rows, :, w:w + 128]
                m, q = jnp.abs(v), v * v
                peak, total = (m, q) if peak is None else (jnp.maximum(peak, m), total + q)
            pieces[t, rows, :] = jnp.max(peak, axis=1)
            pieces[2 + t, rows, :] = jnp.sum(total, axis=1)
            return carry

        lax.fori_loop(0, blocks // 8, measure, 0)
    stat_a[...] = jnp.zeros_like(stat_a)
    for t in range(tensors):
        stat_a[t:t + 1, :] = jnp.max(pieces[t].T, axis=0, keepdims=True)
        stat_a[2 + t:3 + t, :] = jnp.sum(pieces[2 + t].T, axis=0, keepdims=True)
    is_peak = lax.broadcasted_iota(jnp.int32, stat_a.shape, 0) < tensors

    def join(mine, others, n):
        v = mine[...]
        for i in range(n):
            o = others[i]
            v = jnp.where(is_peak, jnp.maximum(v, o), v + o)
        return v


    stage = []
    for d in range(1, cols):
        copy = pltpu.make_async_remote_copy(
            stat_a, all_a.at[d - 1], sa.at[d - 1], ra.at[d - 1],
            device_id={"col": (c + d) % cols}, device_id_type=MESH)
        copy.start()
        stage.append(copy)
    for copy in stage:
        copy.wait()
    stat_b[...] = join(stat_a, all_a, cols - 1)
    stage = []
    for i, d in enumerate(TURNS):
        copy = pltpu.make_async_remote_copy(
            stat_b, all_b.at[i], sb.at[0, i], rb.at[0, i],
            device_id=x_peer(d), device_id_type=MESH)
        copy.start()
        stage.append(copy)

    def pack2(got, offset, dst):
        def step(j, carry):
            k = jnp.minimum(offset + j, slots - 1)
            for s in range(SIDE):
                dst[j, s] = got[s, k]
            return carry

        lax.fori_loop(0, HALF, step, 0)

    second = []
    for t in range(tensors):
        for copy in first[t]:
            copy.wait_recv()
        if t == 1:
            for copy in stage:
                copy.wait()
            stat_c[...] = join(stat_b, all_b, SIDE - 1)
            stage = []
            for i, d in enumerate(TURNS):
                copy = pltpu.make_async_remote_copy(
                    stat_c, all_c.at[i], sb.at[1, i], rb.at[1, i],
                    device_id=y_peer(d), device_id_type=MESH)
                copy.start()
                stage.append(copy)
        for i, d in enumerate(TURNS):
            yd, xd = (y + d) % SIDE, (x + d) % SIDE
            pack2(got_x[t], plan_ref[2 * GROUPS + yd * SIDE + x], out_x.at[t, i])
            copy = pltpu.make_async_remote_copy(
                out_x.at[t, i], x2_ref.at[y, t], send2.at[t, 0, i], recv2.at[t, 0, i],
                device_id=y_peer(d), device_id_type=MESH)
            copy.start()
            second.append(copy)
            pack2(got_y[t], plan_ref[3 * GROUPS + y * SIDE + xd], out_y.at[t, i])
            copy = pltpu.make_async_remote_copy(
                out_y.at[t, i], y2_ref.at[x, t], send2.at[t, 1, i], recv2.at[t, 1, i],
                device_id=x_peer(d), device_id_type=MESH)
            copy.start()
            second.append(copy)
        pack2(got_x[t], plan_ref[2 * GROUPS + me], x2_ref.at[y, t])
        pack2(got_y[t], plan_ref[3 * GROUPS + me], y2_ref.at[x, t])

    for t in range(tensors):
        for copy in first[t]:
            copy.wait_send()
    for copy in stage:
        copy.wait()
    stats_ref[...] = join(stat_c, all_c, SIDE - 1)
    for copy in second:
        copy.wait()


def place_kernel(
    full_size, plan_ref, stats_ref, x2_ref, y2_ref, norm_ref, scale_out, energy_out,
    outb, zeros, inverse, scale_ref, energy_ref, out_sem, small_sem,
):
    tensors, capacity = scale_ref.shape
    me = lax.axis_index("row")
    a, start, n = plan_ref[me], plan_ref[GROUPS + me], plan_ref[4 * GROUPS + me]
    zeros[...] = jnp.zeros_like(zeros)
    rows = zeros.shape[0]

    def put(t, j, src):
        at = pl.ds(pl.multiple_of(j * rows, rows), rows)
        return pltpu.make_async_copy(src, norm_ref.at[t, at], out_sem.at[t, j])

    for t in range(tensors):
        lax.fori_loop(n, capacity, lambda j, _: (put(t, j, zeros).start(), _)[1], 0)

    lanes = stats_ref.shape[1]
    mine = pltpu.roll(stats_ref[...], lax.rem(lanes - start, lanes), 1)
    lane = lax.broadcasted_iota(jnp.int32, mine.shape, 1)
    scale = jnp.where(lane < n, jnp.maximum(mine, 1.0), 1.0)
    energy = jnp.where(lane < n, mine / full_size, 0.0)
    scale_ref[...] = scale[:tensors, :capacity]
    energy_ref[...] = energy[tensors:2 * tensors, :capacity]
    inv = 1.0 / scale
    pick = lax.broadcasted_iota(jnp.int32, (capacity, lanes), 0)
    pick = pick == lax.broadcasted_iota(jnp.int32, (capacity, lanes), 1)
    for t in range(tensors):
        own = jnp.where(pick, jnp.broadcast_to(inv[t:t + 1], pick.shape), 0.0)
        inverse[t] = jnp.broadcast_to(jnp.sum(own, axis=1, keepdims=True), pick.shape)
    small = [
        pltpu.make_async_copy(scale_ref, scale_out, small_sem.at[0]),
        pltpu.make_async_copy(energy_ref, energy_out, small_sem.at[1]),
    ]
    for copy in small:
        copy.start()

    for t in range(tensors):
        def scaled(j, carry, t=t, swap=False):
            factor = jnp.broadcast_to(inverse[t, pl.ds(j, 1), :], (8, lanes))
            for p in range(SIDE):
                for q in range(SIDE):
                    r = (q * SIDE + p) if swap else (p * SIDE + q)
                    for w in range(0, outb.shape[3], lanes):
                        at = slice(w, w + lanes)
                        part = y2_ref[p, t, j - a, q, :, at] if swap else x2_ref[p, t, j, q, :, at]
                        outb[t, j, r * 8:r * 8 + 8, at] = part * factor
            put(t, j, outb.at[t, j]).start()
            return carry

        lax.fori_loop(0, a, functools.partial(scaled, swap=False), 0)
        lax.fori_loop(a, n, functools.partial(scaled, swap=True), 0)
    for t in range(tensors):
        lax.fori_loop(0, capacity, lambda j, _: (put(t, j, zeros).wait(), _)[1], 0)
    for copy in small:
        copy.wait()


def on_device(moments, owner_counts):
    tensors, blocks, sub, width = moments.shape
    groups, cols = lax.axis_size("row"), lax.axis_size("col")
    capacity = 2 * HALF
    f32, i32 = jnp.float32, jnp.int32
    smem = pl.BlockSpec(memory_space=pltpu.SMEM)
    hbm = pl.BlockSpec(memory_space=pl.ANY)
    vmem = pl.BlockSpec(memory_space=pltpu.VMEM)

    plan, tier = pl.pallas_call(
        plan_kernel,
        out_shape=(pltpu.SMEM((128,), i32), pltpu.SMEM((1,), i32)),
        in_specs=[smem],
        out_specs=(smem, smem),
        name="plan",
    )(owner_counts)

    def branch(number, slots):
        arrived = pltpu.VMEM((SIDE, tensors, HALF, SIDE, sub, width), f32)
        got = pltpu.VMEM((SIDE, slots, sub, width), f32)
        sent = pltpu.VMEM((tensors, SIDE - 1, slots, sub, width), f32)
        out = pltpu.VMEM((tensors, SIDE - 1, HALF, SIDE, sub, width), f32)
        stat = pltpu.VMEM((8, blocks), f32)
        dma = pltpu.SemaphoreType.DMA
        peers = max(cols - 1, 1)
        piece = 4 * sub * width
        limit = piece * (2 * blocks + 28 * slots + 48 * HALF) + 1 * 2**20

        def run(moments, plan):
            x2, y2, stats = pl.pallas_call(
                functools.partial(move_kernel, slots, cols),
                out_shape=(arrived, arrived, jax.ShapeDtypeStruct((8, blocks), f32)),
                in_specs=[smem, hbm],
                out_specs=(vmem, vmem, vmem),
                scratch_shapes=[
                    pltpu.VMEM((blocks, sub, width), f32), pltpu.VMEM((blocks, sub, width), f32),
                    sent, sent, got, got, got, got, out, out,
                    pltpu.VMEM((4, blocks, 128), f32), stat, stat, stat,
                    pltpu.VMEM((peers, 8, blocks), f32),
                    pltpu.VMEM((SIDE - 1, 8, blocks), f32),
                    pltpu.VMEM((SIDE - 1, 8, blocks), f32),
                    pltpu.SemaphoreType.REGULAR, dma((2,)), dma((2, 2, 3)), dma((2, 2, 3)), dma((2, 2, 3)), dma((2, 2, 3)),
                    dma((peers,)), dma((peers,)), dma((2, 3)), dma((2, 3)),
                ],
                compiler_params=pltpu.CompilerParams(
                    collective_id=number, has_side_effects=True, vmem_limit_bytes=limit),
                name=f"move{slots}",
            )(plan, moments)
            return pl.pallas_call(
                functools.partial(place_kernel, float(sub * groups * width * cols)),
                out_shape=(
                    jax.ShapeDtypeStruct((tensors, capacity * sub * groups, width), f32),
                    jax.ShapeDtypeStruct((tensors, capacity), f32),
                    jax.ShapeDtypeStruct((tensors, capacity), f32),
                ),
                in_specs=[smem, vmem, vmem, vmem],
                out_specs=(hbm, hbm, hbm),
                scratch_shapes=[
                    pltpu.VMEM((tensors, capacity, sub * groups, width), f32),
                    pltpu.VMEM((sub * groups, width), f32),
                    pltpu.VMEM((tensors, capacity, 128), f32),
                    pltpu.VMEM((tensors, capacity), f32), pltpu.VMEM((tensors, capacity), f32),
                    dma((tensors, capacity)), dma((2,)),
                ],
                compiler_params=pltpu.CompilerParams(vmem_limit_bytes=16 * 2**20),
                name="place",
            )(plan, stats, x2, y2)

        return run

    return lax.switch(tier[0], [branch(i, s) for i, s in enumerate(TIERS)], moments, plan)


def solution(mesh):
    placed = (P(None, None, "row", "col"), P())
    return jax.shard_map(
        on_device,
        mesh=mesh,
        in_specs=placed,
        out_specs=(P(None, "row", "col"), P(None, "row"), P(None, "row")),
        check_vma=False,
    )
```
